128 devices in a mesh: box: 16 (over y, z), panel: 8 (over x, core).
Axes of the slice: x: 4, y: 4, z: 4, core: 2. Of those that a mesh axis runs over, the one named last changes fastest.
Arguments:
- field_start: float32 [4096, 4096], P('box', 'panel'), may hold values from -6 to 6
- fluid_mask: int32 [4096, 4096], P('box', 'panel'), may hold values 0 or 1
- base_visc: float32 [4096, 4096], P('box', 'panel'), may hold values from 0.02 to 0.1
- panel_cell: int32 [16384], P(('box', 'panel')), may hold values from 0 to 131071
- amplitude: bfloat16 [16384, 4096], P('box', 'panel'), may hold values from 0.049804688 to 0.5
- delay_bin: int32 [16384, 4096], P('box', 'panel'), may hold values from 0 to 2044
Outputs:
- field_end: float32 [4096, 4096], P('box', 'panel')
- signals: float32 [4096, 2048], P('panel', 'box')
The draws below stay inside these ranges and needn't reach their ends.
Inputs may be any that keep to these rules, and one draw needn't show every extreme that they name: `panel_cell`: an index, row-major, into the 256 x 512 block of the device that owns the panel.
All inputs are finite; a program needn't handle non-finite values. No bound on the sum of `fluid_mask` on one device may be relied on, other than what follows from the above.
Results may differ from the reference program's by a relative error of at most 0.0029.
Values may be sent and summed in bfloat16 or wider, within the bound.
A program may use at most 64 MiB of HBM per device.

```python
import math
import jax
import jax.numpy as jnp
from jax import lax

CX = 256
CY = 512
PPD = 128
STEPS = 4
OBS = 4096
NB = 2048
NX = 4096
NY = 4096
PANELS = 16384
N_PANEL = 8


def place_ends(array, rng, low, top_value):
    longest = array.shape.index(max(array.shape))
    spots = []
    for shift in (0, 1):
        where = [jax.random.randint(jax.random.fold_in(rng, axis), (), 0, length) for axis, length in enumerate(array.shape)]
        where[longest] = (where[longest] + shift) % array.shape[longest]
        spots.append(tuple(where))
    return array.at[spots[0]].set(low).at[spots[1]].set(top_value)


def level_of(own_key, extent, pieces, least, top_value):
    loudness = 1.0
    for position, shards_of in pieces:
        heights = jax.random.uniform(jax.random.fold_in(jax.random.fold_in(own_key, 6), position), (shards_of,), jnp.float32, least / len(pieces), top_value / len(pieces))
        loudness = loudness * jnp.repeat(jnp.exp(heights), extent[position] // shards_of).reshape((-1,) + (1,) * (len(extent) - 1 - position))
    return loudness


def noise(stream_key, dims, width, most, split=(), kind=jnp.bfloat16):
    drawn = width * jax.random.normal(stream_key, dims, jnp.float32)
    if split:
        drawn = drawn * level_of(stream_key, dims, split, -0.22, 0.18)
    return jnp.clip(drawn, -most, most).astype(kind)


def setup_inputs(seed: int = 0) -> dict:
    seeds = jax.random.split(jax.random.key(seed), 7)
    field_start = noise(seeds[0], (NX, NY), 1.0, 6.0, ((0, 16), (1, 8)), jnp.float32)
    fluid_mask = place_ends((jax.random.randint(seeds[1], (NX, NY), 0, 8) < 7).astype(jnp.int32), jax.random.fold_in(seeds[1], 1), 0, 1)
    base_visc = jnp.clip(jnp.exp(math.log(0.1) - 1.609438 * jax.random.uniform(seeds[2], (NX, NY), jnp.float32) ** level_of(seeds[2], (NX, NY), ((0, 16), (1, 8)), -0.2, 0.2)), 0.02, 0.1)
    panel_cell = place_ends(jax.random.randint(seeds[3], (PANELS,), 0, CX * CY), jax.random.fold_in(seeds[3], 1), 0, (CX * CY) - 1).astype(jnp.int32)
    amplitude = jnp.clip(jnp.exp(math.log(0.5) - 2.306499 * jax.random.uniform(seeds[4], (PANELS, OBS), jnp.float32) ** level_of(seeds[4], (PANELS, OBS), ((0, 16), (1, 8)), -0.2, 0.2)), 0.049804688, 0.5).astype(jnp.bfloat16)
    delay_bin = place_ends(jax.random.randint(seeds[5], (PANELS, OBS), 0, NB - STEPS + 1), jax.random.fold_in(seeds[5], 1), 0, NB - STEPS).astype(jnp.int32)
    return dict(field_start=field_start, fluid_mask=fluid_mask, base_visc=base_visc, panel_cell=panel_cell, amplitude=amplitude, delay_bin=delay_bin)


def advance(ext, mask_c, base_c):
    center = ext[1:-1, 1:-1]
    west = ext[:-2, 1:-1]
    east = ext[2:, 1:-1]
    south = ext[1:-1, :-2]
    north = ext[1:-1, 2:]
    grad_x = 0.5 * (east - west)
    grad_y = 0.5 * (north - south)
    grad_norm = jnp.sqrt(grad_x * grad_x + grad_y * grad_y)
    viscosity = base_c + 0.05 * grad_norm / (1.0 + grad_norm)
    update = center + viscosity * (east + west + north + south - 4.0 * center)
    update = update - 0.15 * (center - west) - 0.1 * (center - south)
    return mask_c * update

def reference(field_start, fluid_mask, base_visc, panel_cell, amplitude, delay_bin):
    owner = (jnp.arange(PANELS, dtype=jnp.int32) // PPD).astype(jnp.int32)
    rows = (owner // N_PANEL * CX + panel_cell // CY).astype(jnp.int32)
    cols = (owner % N_PANEL * CY + panel_cell % CY).astype(jnp.int32)
    maskf = fluid_mask.astype(jnp.float32)
    field = field_start
    taken = []
    for step in range(STEPS):
        field = advance(jnp.pad(field, 1), maskf, base_visc)
        taken.append(field[rows, cols])
    sample = jnp.stack(taken)
    observer_base = (jnp.arange(OBS, dtype=jnp.int32) * NB).astype(jnp.int32)

    def add_block(total, block):
        start = (block * PPD).astype(jnp.int32)
        amp_rows = lax.dynamic_slice_in_dim(amplitude, start, PPD, 0).astype(jnp.float32)
        bin_rows = lax.dynamic_slice_in_dim(delay_bin, start, PPD, 0)
        samp_rows = lax.dynamic_slice_in_dim(sample, start, PPD, 1)
        weight = (amp_rows[None, :, :] * samp_rows[:, :, None]).astype(jnp.bfloat16)
        weight = lax.optimization_barrier(weight).astype(jnp.float32)
        for step in range(STEPS):
            index = (observer_base[None, :] + bin_rows + step).astype(jnp.int32)
            total = total.at[index.reshape(-1)].add(weight[step].reshape(-1))
        return (total, None)
    flat = jnp.zeros((OBS * NB,), jnp.float32)
    flat, unused = lax.scan(add_block, flat, jnp.arange(PANELS // PPD, dtype=jnp.int32))
    return (field, flat.reshape(OBS, NB))
```

```python
import functools

import jax
import jax.numpy as jnp
from jax import lax
from jax.experimental import pallas as pl
from jax.experimental.pallas import tpu as pltpu
from jax.sharding import PartitionSpec as P

MESH = pl.DeviceIdType.MESH
STEPS = 4
NB = 2048
BOX = 16
PAN = 8
ROWS, COLS = 256, 512
PANELS, OBS, OWN = 1024, 512, 128
TOP, FIRST, BOT, EXT_R, EXT_C = 8, 16, 272, 288, 640
RADIX, PARTS, HIGH, LOW = 26, 5, 80, 32
STACK = 4
PER = 8
KT = 256
CHUNK = 64
CHUNKS = OBS // CHUNK
PITCH = CHUNK + 8
TOPINT = 32000.0


def roll(x, shift, axis):
    return pltpu.roll(x, shift % x.shape[axis], axis)


def kernel(
    field, mask, visc, cell, amp, dly, field_out, sig_out,
    ea, eb, em, ev, ledge, redge, got_up, got_dn, mask_up, mask_dn, got_l, got_r, corner,
    samp_own, samp_all, amp_t, high_t, low_t, sb, hist, outbox, scales, inbox, inscales,
    halo_send, halo_recv, samp_send, samp_recv, bin_send, bin_recv, sc_send, sc_recv,
):
    b = lax.axis_index("box")
    p = lax.axis_index("panel")
    has_u, has_d, has_l, has_r = b > 0, b < BOX - 1, p > 0, p < PAN - 1
    diagonals = (
        (has_u & has_l, b - 1, p - 1),
        (has_u & has_r, b - 1, p + 1),
        (has_d & has_l, b + 1, p - 1),
        (has_d & has_r, b + 1, p + 1),
    )

    barrier = pltpu.get_barrier_semaphore()

    def greet(bb, pp):
        pl.semaphore_signal(barrier, inc=1, device_id=(bb, pp), device_id_type=MESH)

    for k in range(1, PAN):
        greet(b, lax.rem(p + k, PAN))
    for k in range(1, BOX):
        greet(lax.rem(b + k, BOX), p)
    expected = jnp.int32(PAN - 1 + BOX - 1)
    for there, bb, pp in diagonals:
        expected = expected + there.astype(jnp.int32)

        @pl.when(there)
        def _(bb=bb, pp=pp):
            greet(bb, pp)

    lane = lax.broadcasted_iota(jnp.int32, (ROWS, 128), 1)
    fe, ve = field[:, :128], visc[:, :128]
    me = mask[:, :128].astype(jnp.float32)
    ledge[...] = jnp.where(
        lane < 4, fe, jnp.where(lane < 8, roll(ve, 4, 1), jnp.where(lane < 12, roll(me, 8, 1), 0.0))
    )
    fe, ve = field[:, COLS - 128 :], visc[:, COLS - 128 :]
    me = mask[:, COLS - 128 :].astype(jnp.float32)
    redge[...] = jnp.where(
        lane >= 124, fe, jnp.where(lane >= 120, roll(ve, -4, 1), jnp.where(lane >= 116, roll(me, -8, 1), 0.0))
    )
    for buf in (ea, eb):
        buf[0:8, :] = jnp.zeros((8, EXT_C), jnp.float32)
        buf[EXT_R - 8 :, :] = jnp.zeros((8, EXT_C), jnp.float32)
    ea[FIRST:BOT, :COLS] = field[...]
    ev[FIRST:BOT, :COLS] = visc[...]
    em[FIRST:BOT, :COLS] = mask[...].astype(jnp.float32)

    def send(i, there, src, dst, bb, pp):
        copy = pltpu.make_async_remote_copy(
            src_ref=src, dst_ref=dst, send_sem=halo_send.at[i], recv_sem=halo_recv.at[i],
            device_id=(bb, pp), device_id_type=MESH,
        )
        return there, copy

    pl.semaphore_wait(barrier, expected)

    lo8, hi8 = pl.ds(0, 8), pl.ds(ROWS - 8, 8)
    halos = (
        (send(0, has_u, field.at[lo8], got_dn.at[0], b - 1, p), has_d),
        (send(1, has_u, visc.at[lo8], got_dn.at[1], b - 1, p), has_d),
        (send(2, has_u, mask.at[lo8], mask_dn, b - 1, p), has_d),
        (send(3, has_d, field.at[hi8], got_up.at[0], b + 1, p), has_u),
        (send(4, has_d, visc.at[hi8], got_up.at[1], b + 1, p), has_u),
        (send(5, has_d, mask.at[hi8], mask_up, b + 1, p), has_u),
        (send(6, has_l, ledge, got_r, b, p - 1), has_r),
        (send(7, has_r, redge, got_l, b, p + 1), has_l),
        (send(8, has_d & has_r, redge.at[hi8], corner.at[0], b + 1, p + 1), has_u & has_l),
        (send(9, has_d & has_l, ledge.at[hi8], corner.at[1], b + 1, p - 1), has_u & has_r),
        (send(10, has_u & has_r, redge.at[lo8], corner.at[2], b - 1, p + 1), has_d & has_l),
        (send(11, has_u & has_l, ledge.at[lo8], corner.at[3], b - 1, p - 1), has_d & has_r),
    )
    for (there, copy), _ in halos:
        pl.when(there)(copy.start)

    def blank(flag, ref):
        @pl.when(jnp.logical_not(flag))
        def _():
            ref[...] = jnp.zeros(ref.shape, ref.dtype)

    blank(has_d, got_dn)
    blank(has_d, mask_dn)
    blank(has_u, got_up)
    blank(has_u, mask_up)
    blank(has_r, got_r)
    blank(has_l, got_l)
    blank(has_u & has_l, corner.at[0])
    blank(has_u & has_r, corner.at[1])
    blank(has_d & has_l, corner.at[2])
    blank(has_d & has_r, corner.at[3])

    def turn(i, _):
        ps = pl.ds(pl.multiple_of(i * 128, 128), 128)
        for c in range(OBS // 128):
            cs = pl.ds(c * 128, 128)
            amp_t[cs, ps] = amp[ps, cs].astype(jnp.float32).T
            d = dly[ps, cs]
            low = d & 127
            r = (low * 79) >> 11
            high_t[cs, ps] = (r * 16 + (d >> 7)).astype(jnp.float32).T
            low_t[cs, ps] = (low - RADIX * r).astype(jnp.float32).T
        return 0

    lax.fori_loop(0, PANELS // 128, turn, 0)

    for (there, copy), comes in halos:
        pl.when(comes)(copy.wait_recv)

    def side(left, right, shift, lane):
        return jnp.where(
            lane < 4, roll(right, -shift, 1), jnp.where(lane >= 124, roll(left, shift, 1), 0.0)
        )

    gl, gr = got_l[...], got_r[...]
    ea[FIRST:BOT, COLS:] = side(gl, gr, 0, lane)
    ev[FIRST:BOT, COLS:] = side(gl, gr, 4, lane)
    em[FIRST:BOT, COLS:] = side(gl, gr, 8, lane)
    lane8 = lax.broadcasted_iota(jnp.int32, (8, 128), 1)
    sub8 = lax.broadcasted_iota(jnp.int32, (8, 128), 0)
    sub_w = lax.broadcasted_iota(jnp.int32, (8, COLS), 0)
    for start, keep, keep_w, got, gmask, cl, cr in (
        (TOP, sub8 >= 4, sub_w >= 4, got_up, mask_up, corner[0], corner[1]),
        (BOT, sub8 < 4, sub_w < 4, got_dn, mask_dn, corner[2], corner[3]),
    ):
        rows = pl.ds(start, 8)
        ea[rows, :COLS] = jnp.where(keep_w, got[0], 0.0)
        ev[rows, :COLS] = jnp.where(keep_w, got[1], 0.0)
        em[rows, :COLS] = jnp.where(keep_w, gmask[...].astype(jnp.float32), 0.0)
        ea[rows, COLS:] = jnp.where(keep, side(cl, cr, 0, lane8), 0.0)
        ev[rows, COLS:] = jnp.where(keep, side(cl, cr, 4, lane8), 0.0)
        em[rows, COLS:] = jnp.where(keep, side(cl, cr, 8, lane8), 0.0)

    crow = cell[...] >> 9
    ccol = cell[...] & (COLS - 1)
    pick_c = jnp.where(
        lax.broadcasted_iota(jnp.int32, (COLS, OWN), 0) == ccol, 1.0, 0.0
    ).astype(jnp.bfloat16)
    pick_r = lax.broadcasted_iota(jnp.int32, (ROWS, OWN), 0) == crow
    samp_own[...] = jnp.zeros_like(samp_own)

    for step in range(STEPS):
        src, dst = (ea, eb) if step % 2 == 0 else (eb, ea)

        def advance(i, _, src=src, dst=dst):
            at = pl.multiple_of(TOP + 16 * i, 8)
            rows = pl.ds(at, 16)
            wide = src[pl.ds(pl.multiple_of(at - 8, 8), 32), :]
            center, west, east = wide[8:24], wide[7:23], wide[9:25]
            south = roll(center, 1, 1)
            north = roll(center, -1, 1)
            grad_x = 0.5 * (east - west)
            grad_y = 0.5 * (north - south)
            grad_norm = jnp.sqrt(grad_x * grad_x + grad_y * grad_y)
            viscosity = ev[rows, :] + 0.05 * grad_norm / (1.0 + grad_norm)
            update = center + viscosity * (east + west + north + south - 4.0 * center)
            update = update - 0.15 * (center - west) - 0.1 * (center - south)
            dst[rows, :] = em[rows, :] * update
            return 0

        lax.fori_loop(0, (EXT_R - 16) // 16, advance, 0)
        now = dst[FIRST:BOT, :COLS]
        high = now.astype(jnp.bfloat16)
        rest = now - high.astype(jnp.float32)
        middle = rest.astype(jnp.bfloat16)
        last = (rest - middle.astype(jnp.float32)).astype(jnp.bfloat16)
        found = jnp.dot(high, pick_c, preferred_element_type=jnp.float32)
        found = found + jnp.dot(middle, pick_c, preferred_element_type=jnp.float32)
        found = found + jnp.dot(last, pick_c, preferred_element_type=jnp.float32)
        samp_own[step : step + 1, :] = jnp.sum(jnp.where(pick_r, found, 0.0), axis=0, keepdims=True)

    field_out[...] = ea[FIRST:BOT, :COLS]

    mine = pl.ds(pl.multiple_of(p * OWN, OWN), OWN)
    samp_all[:, mine] = samp_own[...]

    def samp_copy(k):
        to = lax.rem(p + k, PAN)
        return pltpu.make_async_remote_copy(
            src_ref=samp_own, dst_ref=samp_all.at[:, mine], send_sem=samp_send.at[k],
            recv_sem=samp_recv.at[p], device_id=(b, to), device_id_type=MESH,
        )

    def samp_arrival(k):
        frm = lax.rem(p + k, PAN)
        return pltpu.make_async_remote_copy(
            src_ref=samp_own, dst_ref=samp_all.at[:, pl.ds(pl.multiple_of(frm * OWN, OWN), OWN)],
            send_sem=samp_send.at[k], recv_sem=samp_recv.at[frm], device_id=(b, frm), device_id_type=MESH,
        )

    for k in range(1, PAN):
        samp_copy(k).start()
    for k in range(1, PAN):
        samp_arrival(k).wait_recv()
    for t in range(STEPS):
        sb[t] = jnp.broadcast_to(samp_all[t : t + 1, :], (16, PANELS)).astype(jnp.bfloat16)

    io16 = lax.broadcasted_iota(jnp.int32, (16, KT), 0).astype(jnp.float32)
    lane16 = lax.broadcasted_iota(jnp.int32, (16, 128), 1)
    sub16 = lax.broadcasted_iota(jnp.int32, (16, 128), 0)
    zero = jnp.zeros((16, KT), jnp.bfloat16)

    def bin_group(first, slot):
        acc = None
        for k in range(PANELS // KT):
            ks = pl.ds(k * KT, KT)
            ss = [sb[t, :, ks] for t in range(STEPS)]
            lhs, rhs = [], []
            for i in range(STACK):
                o = pl.ds(first + i, 1)
                hb = jnp.broadcast_to(high_t[o, ks], (16, KT)).astype(jnp.bfloat16)
                ab = jnp.broadcast_to(amp_t[o, ks], (16, KT)).astype(jnp.bfloat16)
                lb = jnp.broadcast_to(low_t[o, ks], (16, KT)).astype(jnp.bfloat16)
                for j in range(HIGH // 16):
                    lhs.append(jnp.where(hb == (io16 + 16 * j).astype(jnp.bfloat16), ab, zero))
                for j in range(LOW // 16):
                    v = zero
                    for t in range(STEPS):
                        v = jnp.where(lb == (io16 + (16 * j - t)).astype(jnp.bfloat16), ss[t], v)
                    rhs.append(v)
            part = lax.dot_general(
                jnp.concatenate(lhs, 0), jnp.concatenate(rhs, 0), (((1,), (1,)), ((), ())),
                preferred_element_type=jnp.float32,
            )
            acc = part if acc is None else acc + part
        for i in range(STACK):
            total = None
            for r in range(PARTS):
                blk = acc[i * HIGH + 16 * r : i * HIGH + 16 * r + 16, :]
                blk = jnp.where((lane16 >= LOW * i) & (lane16 < LOW * i + LOW), blk, 0.0)
                if (RADIX * r - LOW * i) % 128:
                    blk = roll(blk, RADIX * r - LOW * i, 1)
                if r == PARTS - 1:
                    over = jnp.where((lane16 < 8) & (sub16 < 15), blk, 0.0)
                    blk = jnp.where(lane16 < 8, 0.0, blk) + roll(over, 1, 0)
                total = blk if total is None else total + blk
            hist[pl.ds(slot + i, 16, stride=PITCH), :] = total

    def bin_copy(k, c):
        to = lax.rem(b + k, BOX)
        rows = pl.ds(pl.multiple_of(c * CHUNK, CHUNK), CHUNK)
        return pltpu.make_async_remote_copy(
            src_ref=outbox.at[to, rows], dst_ref=inbox.at[b, rows], send_sem=bin_send.at[k, c],
            recv_sem=bin_recv.at[b, c], device_id=(to, p), device_id_type=MESH,
        )

    def bin_arrival(k, c):
        frm = lax.rem(b + k, BOX)
        rows = pl.ds(pl.multiple_of(c * CHUNK, CHUNK), CHUNK)
        return pltpu.make_async_remote_copy(
            src_ref=outbox.at[frm, rows], dst_ref=inbox.at[frm, rows], send_sem=bin_send.at[k, c],
            recv_sem=bin_recv.at[frm, c], device_id=(frm, p), device_id_type=MESH,
        )

    def scale_copy(k):
        to = lax.rem(b + k, BOX)
        return pltpu.make_async_remote_copy(
            src_ref=scales.at[to], dst_ref=inscales.at[b], send_sem=sc_send.at[k],
            recv_sem=sc_recv.at[b], device_id=(to, p), device_id_type=MESH,
        )

    def scale_arrival(k):
        frm = lax.rem(b + k, BOX)
        return pltpu.make_async_remote_copy(
            src_ref=scales.at[frm], dst_ref=inscales.at[frm], send_sem=sc_send.at[k],
            recv_sem=sc_recv.at[frm], device_id=(frm, p), device_id_type=MESH,
        )

    def chunk(c, _):
        def some(g, _):
            for u in range(PER):
                slot = (g * PER + u) * STACK
                bin_group(c * CHUNK + slot, slot)
            return 0

        lax.fori_loop(0, CHUNK // (STACK * PER), some, 0)
        rows = pl.ds(pl.multiple_of(c * CHUNK, CHUNK), CHUNK)
        for q in range(BOX):
            x = hist[q * PITCH : q * PITCH + CHUNK, :]
            most = jnp.max(jnp.max(jnp.abs(x), axis=0, keepdims=True), axis=1, keepdims=True)
            most = jnp.maximum(jnp.broadcast_to(most, (1, 128)), 1e-30)
            y = jnp.floor(x * (TOPINT / most) + 0.5)
            outbox[q, rows, :] = y.astype(jnp.int32).astype(jnp.int16)
            scales[q, pl.ds(c, 1), :] = most * (1.0 / TOPINT)
        for k in range(1, BOX):
            bin_copy(k, c).start()
        inbox[b, rows, :] = outbox[b, rows, :]
        return 0

    lax.fori_loop(0, CHUNKS, chunk, 0)
    for k in range(1, BOX):
        scale_copy(k).start()
    inscales[b] = scales[b]

    def arrive(k, _):
        scale_arrival(k).wait_recv()
        for c in range(CHUNKS):
            bin_arrival(k, c).wait_recv()
        return 0

    lax.fori_loop(1, BOX, arrive, 0)

    def gather(c, _):
        rows = pl.ds(pl.multiple_of(c * CHUNK, CHUNK), CHUNK)
        total = None
        for s in range(BOX):
            x = inbox[s, rows, :].astype(jnp.int32).astype(jnp.float32) * inscales[s, pl.ds(c, 1), :]
            total = x if total is None else total + x
        sig_out[rows, :] = total
        return 0

    lax.fori_loop(0, CHUNKS, gather, 0)

    for (there, copy), _ in halos:
        pl.when(there)(copy.wait_send)
    for k in range(1, PAN):
        samp_copy(k).wait_send()

    def sent(k, _):
        scale_copy(k).wait_send()
        for c in range(CHUNKS):
            bin_copy(k, c).wait_send()
        return 0

    lax.fori_loop(1, BOX, sent, 0)


def on_device(field_start, fluid_mask, base_visc, panel_cell, amplitude, delay_bin):
    f32, bf16, i32 = jnp.float32, jnp.bfloat16, jnp.int32
    vmem = lambda shape, dtype=f32: pltpu.VMEM(shape, dtype)
    dma = lambda *shape: pltpu.SemaphoreType.DMA(shape)
    scratch = [
        vmem((EXT_R, EXT_C)), vmem((EXT_R, EXT_C)), vmem((EXT_R, EXT_C)), vmem((EXT_R, EXT_C)),
        vmem((ROWS, 128)), vmem((ROWS, 128)),
        vmem((2, 8, COLS)), vmem((2, 8, COLS)), vmem((8, COLS), i32), vmem((8, COLS), i32),
        vmem((ROWS, 128)), vmem((ROWS, 128)), vmem((4, 8, 128)),
        vmem((8, OWN)), vmem((8, PANELS)),
        vmem((OBS, PANELS)), vmem((OBS, PANELS)), vmem((OBS, PANELS)),
        vmem((STEPS, 16, PANELS), bf16),
        vmem((BOX * PITCH, 128)),
        vmem((BOX, OBS, 128), jnp.int16), vmem((BOX, CHUNKS, 128)),
        vmem((BOX, OBS, 128), jnp.int16), vmem((BOX, CHUNKS, 128)),
        dma(12), dma(12), dma(PAN), dma(PAN), dma(BOX, CHUNKS), dma(BOX, CHUNKS), dma(BOX), dma(BOX),
    ]
    return pl.pallas_call(
        kernel,
        out_shape=(
            jax.ShapeDtypeStruct((ROWS, COLS), f32),
            jax.ShapeDtypeStruct((OBS, NB // BOX), f32),
        ),
        in_specs=[pl.BlockSpec(memory_space=pltpu.VMEM)] * 6,
        out_specs=(pl.BlockSpec(memory_space=pltpu.VMEM),) * 2,
        scratch_shapes=scratch,
        compiler_params=pltpu.CompilerParams(
            collective_id=0, has_side_effects=True, vmem_limit_bytes=56 * 2**20
        ),
    )(field_start, fluid_mask, base_visc, panel_cell.reshape(1, OWN), amplitude, delay_bin)


def solution(mesh):
    placed = (
        P("box", "panel"),
        P("box", "panel"),
        P("box", "panel"),
        P(("box", "panel")),
        P("box", "panel"),
        P("box", "panel"),
    )
    return jax.shard_map(
        on_device,
        mesh=mesh,
        in_specs=placed,
        out_specs=(P("box", "panel"), P("panel", "box")),
        check_vma=False,
    )
```

```python
import functools

import jax
import jax.numpy as jnp
from jax import lax
from jax.experimental import pallas as pl
from jax.experimental.pallas import tpu as pltpu
from jax.sharding import PartitionSpec as P

MESH = pl.DeviceIdType.MESH
STEPS = 4
NB = 2048
BOX = 16
PAN = 8
ROWS, COLS = 256, 512
PANELS, OBS, OWN = 1024, 512, 128
TOP, FIRST, BOT, EXT_R, EXT_C = 8, 16, 272, 304, 640
STRIP = 32
RADIX, PARTS, HIGH, LOW = 26, 5, 80, 32
STACK = 4
KT = 256
EARLY = 3
CHUNK = 64
CHUNKS = OBS // CHUNK
PITCH = CHUNK + 8
TOPINT = 32000.0


def roll(x, shift, axis):
    return pltpu.roll(x, shift % x.shape[axis], axis)


def kernel(
    field_in, mask_in, visc_in, cell_in, amp_in, dly_in, field_out, sig_out,
    mask, cell, amp, dly, ea, eb, em, ev, ledge, redge, got_up, got_dn, mask_up, mask_dn, got_l, got_r, corner,
    samp_own, samp_all, amp_t, high_t, low_t, sb, hist, outbox, scales, inbox, inscales,
    loads, store, halo_send, halo_recv, samp_send, samp_recv, bin_send, bin_recv, sc_send, sc_recv,
):
    b = lax.axis_index("box")
    p = lax.axis_index("panel")
    has_u, has_d, has_l, has_r = b > 0, b < BOX - 1, p > 0, p < PAN - 1
    diagonals = (
        (has_u & has_l, b - 1, p - 1),
        (has_u & has_r, b - 1, p + 1),
        (has_d & has_l, b + 1, p - 1),
        (has_d & has_r, b + 1, p + 1),
    )

    own_rows, own_cols = pl.ds(FIRST, ROWS), pl.ds(0, COLS)
    arrivals = [
        pltpu.make_async_copy(src, dst, loads.at[i])
        for i, (src, dst) in enumerate((
            (field_in, ea.at[own_rows, own_cols]), (visc_in, ev.at[own_rows, own_cols]),
            (mask_in, mask), (cell_in, cell), (amp_in, amp), (dly_in, dly),
        ))
    ]
    for copy in arrivals:
        copy.start()

    barrier = pltpu.get_barrier_semaphore()

    def greet(bb, pp):
        pl.semaphore_signal(barrier, inc=1, device_id=(bb, pp), device_id_type=MESH)

    for k in range(1, PAN):
        greet(b, lax.rem(p + k, PAN))
    for k in range(1, BOX):
        greet(lax.rem(b + k, BOX), p)
    expected = jnp.int32(PAN - 1 + BOX - 1)
    for there, bb, pp in diagonals:
        expected = expected + there.astype(jnp.int32)

        @pl.when(there)
        def _(bb=bb, pp=pp):
            greet(bb, pp)

    for buf in (ea, eb, ev, em):
        buf[0:8, :] = jnp.zeros((8, EXT_C), jnp.float32)
        buf[BOT + 8 :, :] = jnp.zeros((EXT_R - BOT - 8, EXT_C), jnp.float32)
    hist[...] = jnp.zeros_like(hist)
    samp_own[...] = jnp.zeros_like(samp_own)
    for copy in arrivals[:4]:
        copy.wait()

    lane = lax.broadcasted_iota(jnp.int32, (ROWS, 128), 1)
    fe, ve = ea[own_rows, :128], ev[own_rows, :128]
    me = mask[:, :128].astype(jnp.float32)
    ledge[...] = jnp.where(
        lane < 4, fe, jnp.where(lane < 8, roll(ve, 4, 1), jnp.where(lane < 12, roll(me, 8, 1), 0.0))
    )
    fe, ve = ea[own_rows, COLS - 128 : COLS], ev[own_rows, COLS - 128 : COLS]
    me = mask[:, COLS - 128 :].astype(jnp.float32)
    redge[...] = jnp.where(
        lane >= 124, fe, jnp.where(lane >= 120, roll(ve, -4, 1), jnp.where(lane >= 116, roll(me, -8, 1), 0.0))
    )
    em[own_rows, :COLS] = mask[...].astype(jnp.float32)
    for copy in arrivals[4:]:
        copy.wait()

    def turn(i, _):
        ps = pl.ds(pl.multiple_of(i * 128, 128), 128)
        for c in range(OBS // 128):
            cs = pl.ds(c * 128, 128)
            amp_t[cs, ps] = amp[ps, cs].astype(jnp.float32).T
            d = dly[ps, cs]
            low = d & 127
            r = (low * 79) >> 11
            high_t[cs, ps] = (r * 16 + (d >> 7)).astype(jnp.float32).T
            low_t[cs, ps] = (low - RADIX * r).astype(jnp.float32).T
        return 0

    lax.fori_loop(0, EARLY, turn, 0)

    def send(i, there, src, dst, bb, pp):
        copy = pltpu.make_async_remote_copy(
            src_ref=src, dst_ref=dst, send_sem=halo_send.at[i], recv_sem=halo_recv.at[i],
            device_id=(bb, pp), device_id_type=MESH,
        )
        return there, copy

    pl.semaphore_wait(barrier, expected)

    lo8, hi8 = pl.ds(0, 8), pl.ds(ROWS - 8, 8)
    lo_own, hi_own = pl.ds(FIRST, 8), pl.ds(BOT - 8, 8)
    halos = (
        (send(0, has_u, ea.at[lo_own, own_cols], got_dn.at[0], b - 1, p), has_d),
        (send(1, has_u, ev.at[lo_own, own_cols], got_dn.at[1], b - 1, p), has_d),
        (send(2, has_u, mask.at[lo8], mask_dn, b - 1, p), has_d),
        (send(3, has_d, ea.at[hi_own, own_cols], got_up.at[0], b + 1, p), has_u),
        (send(4, has_d, ev.at[hi_own, own_cols], got_up.at[1], b + 1, p), has_u),
        (send(5, has_d, mask.at[hi8], mask_up, b + 1, p), has_u),
        (send(6, has_l, ledge, got_r, b, p - 1), has_r),
        (send(7, has_r, redge, got_l, b, p + 1), has_l),
        (send(8, has_d & has_r, redge.at[hi8], corner.at[0], b + 1, p + 1), has_u & has_l),
        (send(9, has_d & has_l, ledge.at[hi8], corner.at[1], b + 1, p - 1), has_u & has_r),
        (send(10, has_u & has_r, redge.at[lo8], corner.at[2], b - 1, p + 1), has_d & has_l),
        (send(11, has_u & has_l, ledge.at[lo8], corner.at[3], b - 1, p - 1), has_d & has_r),
    )
    for (there, copy), _ in halos:
        pl.when(there)(copy.start)

    def blank(flag, ref):
        @pl.when(jnp.logical_not(flag))
        def _():
            ref[...] = jnp.zeros(ref.shape, ref.dtype)

    blank(has_d, got_dn)
    blank(has_d, mask_dn)
    blank(has_u, got_up)
    blank(has_u, mask_up)
    blank(has_r, got_r)
    blank(has_l, got_l)
    blank(has_u & has_l, corner.at[0])
    blank(has_u & has_r, corner.at[1])
    blank(has_d & has_l, corner.at[2])
    blank(has_d & has_r, corner.at[3])

    lax.fori_loop(EARLY, PANELS // 128, turn, 0)

    for (there, copy), comes in halos:
        pl.when(comes)(copy.wait_recv)
        pl.when(there)(copy.wait_send)

    def side(left, right, shift, lane):
        return jnp.where(
            lane < 4, roll(right, -shift, 1), jnp.where(lane >= 124, roll(left, shift, 1), 0.0)
        )

    gl, gr = got_l[...], got_r[...]
    ea[FIRST:BOT, COLS:] = side(gl, gr, 0, lane)
    ev[FIRST:BOT, COLS:] = side(gl, gr, 4, lane)
    em[FIRST:BOT, COLS:] = side(gl, gr, 8, lane)
    lane8 = lax.broadcasted_iota(jnp.int32, (8, 128), 1)
    sub8 = lax.broadcasted_iota(jnp.int32, (8, 128), 0)
    sub_w = lax.broadcasted_iota(jnp.int32, (8, COLS), 0)
    for start, keep, keep_w, got, gmask, cl, cr in (
        (TOP, sub8 >= 4, sub_w >= 4, got_up, mask_up, corner[0], corner[1]),
        (BOT, sub8 < 4, sub_w < 4, got_dn, mask_dn, corner[2], corner[3]),
    ):
        rows = pl.ds(start, 8)
        ea[rows, :COLS] = jnp.where(keep_w, got[0], 0.0)
        ev[rows, :COLS] = jnp.where(keep_w, got[1], 0.0)
        em[rows, :COLS] = jnp.where(keep_w, gmask[...].astype(jnp.float32), 0.0)
        ea[rows, COLS:] = jnp.where(keep, side(cl, cr, 0, lane8), 0.0)
        ev[rows, COLS:] = jnp.where(keep, side(cl, cr, 4, lane8), 0.0)
        em[rows, COLS:] = jnp.where(keep, side(cl, cr, 8, lane8), 0.0)

    crow = cell[...] >> 9
    ccol = cell[...] & (COLS - 1)
    pick_c = jnp.where(
        lax.broadcasted_iota(jnp.int32, (COLS, OWN), 0) == ccol, 1.0, 0.0
    ).astype(jnp.bfloat16)
    pick_r = lax.broadcasted_iota(jnp.int32, (ROWS, OWN), 0) == crow
    for step in range(STEPS):
        src, dst = (ea, eb) if step % 2 == 0 else (eb, ea)

        def advance(i, _, src=src, dst=dst):
            at = pl.multiple_of(TOP + STRIP * i, 8)
            rows = pl.ds(at, STRIP)
            wide = src[pl.ds(pl.multiple_of(at - 8, 8), STRIP + 16), :]
            center = wide[8 : STRIP + 8]
            west = roll(wide, 1, 0)[8 : STRIP + 8]
            east = roll(wide, -1, 0)[8 : STRIP + 8]
            south = roll(center, 1, 1)
            north = roll(center, -1, 1)
            grad_x = 0.5 * (east - west)
            grad_y = 0.5 * (north - south)
            grad_norm = jnp.sqrt(grad_x * grad_x + grad_y * grad_y)
            viscosity = ev[rows, :] + 0.05 * grad_norm / (1.0 + grad_norm)
            update = center + viscosity * (east + west + north + south - 4.0 * center)
            update = update - 0.15 * (center - west) - 0.1 * (center - south)
            dst[rows, :] = em[rows, :] * update
            return 0

        lax.fori_loop(0, (EXT_R - 16) // STRIP, advance, 0)
        found = jnp.dot(
            dst[FIRST:BOT, :COLS].astype(jnp.bfloat16), pick_c, preferred_element_type=jnp.float32
        )
        samp_own[step : step + 1, :] = jnp.sum(jnp.where(pick_r, found, 0.0), axis=0, keepdims=True)

    out = pltpu.make_async_copy(ea.at[own_rows, own_cols], field_out, store)
    out.start()

    mine = pl.ds(pl.multiple_of(p * OWN, OWN), OWN)
    samp_all[:, mine] = samp_own[...]

    def samp_copy(k):
        to = lax.rem(p + k, PAN)
        return pltpu.make_async_remote_copy(
            src_ref=samp_own, dst_ref=samp_all.at[:, mine], send_sem=samp_send.at[k],
            recv_sem=samp_recv.at[p], device_id=(b, to), device_id_type=MESH,
        )

    def samp_arrival(k):
        frm = lax.rem(p + k, PAN)
        return pltpu.make_async_remote_copy(
            src_ref=samp_own, dst_ref=samp_all.at[:, pl.ds(pl.multiple_of(frm * OWN, OWN), OWN)],
            send_sem=samp_send.at[k], recv_sem=samp_recv.at[frm], device_id=(b, frm), device_id_type=MESH,
        )

    for k in range(1, PAN):
        samp_copy(k).start()
    for k in range(1, PAN):
        samp_arrival(k).wait_recv()
    for t in range(STEPS):
        sb[t] = jnp.broadcast_to(samp_all[t : t + 1, :], (16, PANELS)).astype(jnp.bfloat16)

    io16 = lax.broadcasted_iota(jnp.int32, (16, KT), 0).astype(jnp.float32)
    lane16 = lax.broadcasted_iota(jnp.int32, (16, 128), 1)
    sub16 = lax.broadcasted_iota(jnp.int32, (16, 128), 0)
    zero = jnp.zeros((16, KT), jnp.bfloat16)

    def bin_group(first, slot):
        acc = None
        for k in range(PANELS // KT):
            ks = pl.ds(k * KT, KT)
            ss = [sb[t, :, ks] for t in range(STEPS)]
            lhs, rhs = [], []
            for i in range(STACK):
                o = pl.ds(first + i, 1)
                hb = jnp.broadcast_to(high_t[o, ks], (16, KT)).astype(jnp.bfloat16)
                ab = jnp.broadcast_to(amp_t[o, ks], (16, KT)).astype(jnp.bfloat16)
                lb = jnp.broadcast_to(low_t[o, ks], (16, KT)).astype(jnp.bfloat16)
                for j in range(HIGH // 16):
                    lhs.append(jnp.where(hb == (io16 + 16 * j).astype(jnp.bfloat16), ab, zero))
                for j in range(LOW // 16):
                    v = zero
                    for t in range(STEPS):
                        v = jnp.where(lb == (io16 + (16 * j - t)).astype(jnp.bfloat16), ss[t], v)
                    rhs.append(v)
            part = lax.dot_general(
                jnp.concatenate(lhs, 0), jnp.concatenate(rhs, 0), (((1,), (1,)), ((), ())),
                preferred_element_type=jnp.float32,
            )
            acc = part if acc is None else acc + part
        for i in range(STACK):
            total = None
            for r in range(PARTS):
                blk = acc[i * HIGH + 16 * r : i * HIGH + 16 * r + 16, :]
                blk = jnp.where((lane16 >= LOW * i) & (lane16 < LOW * i + LOW), blk, 0.0)
                if (RADIX * r - LOW * i) % 128:
                    blk = roll(blk, RADIX * r - LOW * i, 1)
                if r == PARTS - 1:
                    over = jnp.where((lane16 < 8) & (sub16 < 15), blk, 0.0)
                    blk = jnp.where(lane16 < 8, 0.0, blk) + roll(over, 1, 0)
                total = blk if total is None else total + blk
            hist[pl.ds(slot + i, 16, stride=PITCH), :] = total

    def bin_copy(k, c):
        to = lax.rem(b + k, BOX)
        rows = pl.ds(pl.multiple_of(c * CHUNK, CHUNK), CHUNK)
        return pltpu.make_async_remote_copy(
            src_ref=outbox.at[to, rows], dst_ref=inbox.at[b, rows], send_sem=bin_send.at[k],
            recv_sem=bin_recv.at[b], device_id=(to, p), device_id_type=MESH,
        )

    def bin_whole(k):
        frm = lax.rem(b + k, BOX)
        return pltpu.make_async_remote_copy(
            src_ref=outbox.at[frm], dst_ref=inbox.at[frm], send_sem=bin_send.at[k],
            recv_sem=bin_recv.at[frm], device_id=(frm, p), device_id_type=MESH,
        )

    def scale_copy(k):
        to = lax.rem(b + k, BOX)
        return pltpu.make_async_remote_copy(
            src_ref=scales.at[to], dst_ref=inscales.at[b], send_sem=sc_send.at[k],
            recv_sem=sc_recv.at[b], device_id=(to, p), device_id_type=MESH,
        )

    def scale_arrival(k):
        frm = lax.rem(b + k, BOX)
        return pltpu.make_async_remote_copy(
            src_ref=scales.at[frm], dst_ref=inscales.at[frm], send_sem=sc_send.at[k],
            recv_sem=sc_recv.at[frm], device_id=(frm, p), device_id_type=MESH,
        )

    def pack(c, base):
        rows = pl.ds(pl.multiple_of(c * CHUNK, CHUNK), CHUNK)
        for q in range(BOX):
            x = hist[pl.ds(pl.multiple_of(base + q * PITCH, 8), CHUNK), :]
            most = jnp.max(jnp.max(jnp.abs(x), axis=0, keepdims=True), axis=1, keepdims=True)
            most = jnp.maximum(jnp.broadcast_to(most, (1, 128)), 1e-30)
            y = jnp.floor(x * (TOPINT / most) + 0.5)
            outbox[q, rows, :] = y.astype(jnp.int32).astype(jnp.int16)
            scales[q, pl.ds(c, 1), :] = most * (1.0 / TOPINT)

    def post(c):
        rows = pl.ds(pl.multiple_of(c * CHUNK, CHUNK), CHUNK)
        for k in range(1, BOX):
            bin_copy(k, c).start()
        inbox[b, rows, :] = outbox[b, rows, :]

    def chunk(c, _):
        before = jnp.maximum(c - 1, 0)
        side = lax.rem(c, 2) * (BOX * PITCH)
        pack(before, BOX * PITCH - side)
        for u in range(CHUNK // STACK):
            bin_group(c * CHUNK + u * STACK, side + u * STACK)

        @pl.when(c > 0)
        def _():
            post(before)

        return 0

    lax.fori_loop(0, CHUNKS, chunk, 0)
    pack(CHUNKS - 1, (CHUNKS - 1) % 2 * (BOX * PITCH))
    post(CHUNKS - 1)
    for k in range(1, BOX):
        scale_copy(k).start()
    inscales[b] = scales[b]

    def arrive(k, _):
        scale_arrival(k).wait_recv()
        bin_whole(k).wait_recv()
        return 0

    lax.fori_loop(1, BOX, arrive, 0)

    def gather(c, _):
        rows = pl.ds(pl.multiple_of(c * CHUNK, CHUNK), CHUNK)
        total = None
        for s in range(BOX):
            x = inbox[s, rows, :].astype(jnp.int32).astype(jnp.float32) * inscales[s, pl.ds(c, 1), :]
            total = x if total is None else total + x
        sig_out[rows, :] = total
        return 0

    lax.fori_loop(0, CHUNKS, gather, 0)

    out.wait()
    for k in range(1, PAN):
        samp_copy(k).wait_send()

    def sent(k, _):
        scale_copy(k).wait_send()
        bin_whole(k).wait_send()
        return 0

    lax.fori_loop(1, BOX, sent, 0)


def on_device(field_start, fluid_mask, base_visc, panel_cell, amplitude, delay_bin):
    f32, bf16, i32 = jnp.float32, jnp.bfloat16, jnp.int32
    vmem = lambda shape, dtype=f32: pltpu.VMEM(shape, dtype)
    dma = lambda *shape: pltpu.SemaphoreType.DMA(shape)
    scratch = [
        vmem((ROWS, COLS), i32), vmem((1, OWN), i32), vmem((PANELS, OBS), bf16), vmem((PANELS, OBS), i32),
        vmem((EXT_R, EXT_C)), vmem((EXT_R, EXT_C)), vmem((EXT_R, EXT_C)), vmem((EXT_R, EXT_C)),
        vmem((ROWS, 128)), vmem((ROWS, 128)),
        vmem((2, 8, COLS)), vmem((2, 8, COLS)), vmem((8, COLS), i32), vmem((8, COLS), i32),
        vmem((ROWS, 128)), vmem((ROWS, 128)), vmem((4, 8, 128)),
        vmem((8, OWN)), vmem((8, PANELS)),
        vmem((OBS, PANELS)), vmem((OBS, PANELS)), vmem((OBS, PANELS)),
        vmem((STEPS, 16, PANELS), bf16),
        vmem((2 * BOX * PITCH, 128)),
        vmem((BOX, OBS, 128), jnp.int16), vmem((BOX, CHUNKS, 128)),
        vmem((BOX, OBS, 128), jnp.int16), vmem((BOX, CHUNKS, 128)),
        dma(6), pltpu.SemaphoreType.DMA, dma(12), dma(12), dma(PAN), dma(PAN), dma(BOX), dma(BOX), dma(BOX), dma(BOX),
    ]
    return pl.pallas_call(
        kernel,
        out_shape=(
            jax.ShapeDtypeStruct((ROWS, COLS), f32),
            jax.ShapeDtypeStruct((OBS, NB // BOX), f32),
        ),
        in_specs=[pl.BlockSpec(memory_space=pl.ANY)] * 6,
        out_specs=(pl.BlockSpec(memory_space=pl.ANY), pl.BlockSpec(memory_space=pltpu.VMEM)),
        scratch_shapes=scratch,
        compiler_params=pltpu.CompilerParams(
            collective_id=0, has_side_effects=True, vmem_limit_bytes=56 * 2**20
        ),
    )(field_start, fluid_mask, base_visc, panel_cell.reshape(1, OWN), amplitude, delay_bin)


def solution(mesh):
    placed = (
        P("box", "panel"),
        P("box", "panel"),
        P("box", "panel"),
        P(("box", "panel")),
        P("box", "panel"),
        P("box", "panel"),
    )
    return jax.shard_map(
        on_device,
        mesh=mesh,
        in_specs=placed,
        out_specs=(P("box", "panel"), P("panel", "box")),
        check_vma=False,
    )
```

```python
import functools

import jax
import jax.numpy as jnp
from jax import lax
from jax.experimental import pallas as pl
from jax.experimental.pallas import tpu as pltpu
from jax.sharding import PartitionSpec as P

MESH = pl.DeviceIdType.MESH
STEPS = 4
NB = 2048
BOX = 16
PAN = 8
ROWS, COLS = 256, 512
PANELS, OBS, OWN = 1024, 512, 128
TOP, FIRST, BOT, EXT_R, EXT_C = 8, 16, 272, 304, 640
STRIP = 96
RADIX, PARTS, HIGH, LOW = 26, 5, 80, 32
STACK = 4
KT = 256
EARLY = 3
CHUNK = 64
CHUNKS = OBS // CHUNK
HALF = CHUNK // 2
HALVES = OBS // HALF
PITCH = CHUNK + 8
TOPINT = 32000.0
ORDER = (10, 9, 11, 6, 14, 8, 2, 5, 7, 13, 15, 12, 4, 3, 1)


def roll(x, shift, axis):
    return pltpu.roll(x, shift % x.shape[axis], axis)


def kernel(
    field_in, mask_in, visc_in, cell_in, amp_in, dly_in, field_out, sig_out,
    mask, cell, amp, dly, ea, eb, em, ev, ledge, redge, got_up, got_dn, mask_up, mask_dn, got_l, got_r, corner,
    samp_own, samp_all, amp_t, high_t, low_t, sb, hist, outbox, scales, scale_out, inbox, inscales, units,
    loads, store, halo_send, halo_recv, samp_send, samp_recv, bin_send, bin_recv, sc_send, sc_recv,
):
    b = lax.axis_index("box")
    p = lax.axis_index("panel")
    has_u, has_d, has_l, has_r = b > 0, b < BOX - 1, p > 0, p < PAN - 1
    diagonals = (
        (has_u & has_l, b - 1, p - 1),
        (has_u & has_r, b - 1, p + 1),
        (has_d & has_l, b + 1, p - 1),
        (has_d & has_r, b + 1, p + 1),
    )

    own_rows, own_cols = pl.ds(FIRST, ROWS), pl.ds(0, COLS)
    arrivals = [
        pltpu.make_async_copy(src, dst, loads.at[i])
        for i, (src, dst) in enumerate((
            (field_in, ea.at[own_rows, own_cols]), (visc_in, ev.at[own_rows, own_cols]),
            (mask_in, mask), (cell_in, cell), (amp_in, amp), (dly_in, dly),
        ))
    ]
    for copy in arrivals:
        copy.start()

    barrier = pltpu.get_barrier_semaphore()

    def greet(bb, pp):
        pl.semaphore_signal(barrier, inc=1, device_id=(bb, pp), device_id_type=MESH)

    for k in range(1, PAN):
        greet(b, lax.rem(p + k, PAN))
    for k in range(1, BOX):
        greet(lax.rem(b + k, BOX), p)
    expected = jnp.int32(PAN - 1 + BOX - 1)
    for there, bb, pp in diagonals:
        expected = expected + there.astype(jnp.int32)

        @pl.when(there)
        def _(bb=bb, pp=pp):
            greet(bb, pp)

    for buf in (ea, eb, ev, em):
        buf[0:8, :] = jnp.zeros((8, EXT_C), jnp.float32)
        buf[BOT + 8 :, :] = jnp.zeros((EXT_R - BOT - 8, EXT_C), jnp.float32)
    hist[...] = jnp.zeros_like(hist)
    samp_own[...] = jnp.zeros_like(samp_own)
    for copy in arrivals[:4]:
        copy.wait()

    lane = lax.broadcasted_iota(jnp.int32, (ROWS, 128), 1)
    fe, ve = ea[own_rows, :128], ev[own_rows, :128]
    me = mask[:, :128].astype(jnp.float32)
    ledge[...] = jnp.where(
        lane < 4, fe, jnp.where(lane < 8, roll(ve, 4, 1), jnp.where(lane < 12, roll(me, 8, 1), 0.0))
    )
    fe, ve = ea[own_rows, COLS - 128 : COLS], ev[own_rows, COLS - 128 : COLS]
    me = mask[:, COLS - 128 :].astype(jnp.float32)
    redge[...] = jnp.where(
        lane >= 124, fe, jnp.where(lane >= 120, roll(ve, -4, 1), jnp.where(lane >= 116, roll(me, -8, 1), 0.0))
    )
    em[own_rows, :COLS] = mask[...].astype(jnp.float32)
    for copy in arrivals[4:]:
        copy.wait()

    def turn(i, _):
        ps = pl.ds(pl.multiple_of(i * 128, 128), 128)
        for c in range(OBS // 128):
            cs = pl.ds(c * 128, 128)
            amp_t[cs, ps] = amp[ps, cs].astype(jnp.float32).T
            d = dly[ps, cs]
            low = d & 127
            r = (low * 79) >> 11
            high_t[cs, ps] = (r * 16 + (d >> 7)).astype(jnp.float32).T
            low_t[cs, ps] = (low - RADIX * r).astype(jnp.float32).T
        return 0

    lax.fori_loop(0, EARLY, turn, 0)

    def send(i, there, src, dst, bb, pp):
        copy = pltpu.make_async_remote_copy(
            src_ref=src, dst_ref=dst, send_sem=halo_send.at[i], recv_sem=halo_recv.at[i],
            device_id=(bb, pp), device_id_type=MESH,
        )
        return there, copy

    pl.semaphore_wait(barrier, expected)

    lo8, hi8 = pl.ds(0, 8), pl.ds(ROWS - 8, 8)
    lo_own, hi_own = pl.ds(FIRST, 8), pl.ds(BOT - 8, 8)
    halos = (
        (send(0, has_u, ea.at[lo_own, own_cols], got_dn.at[0], b - 1, p), has_d),
        (send(1, has_u, ev.at[lo_own, own_cols], got_dn.at[1], b - 1, p), has_d),
        (send(2, has_u, mask.at[lo8], mask_dn, b - 1, p), has_d),
        (send(3, has_d, ea.at[hi_own, own_cols], got_up.at[0], b + 1, p), has_u),
        (send(4, has_d, ev.at[hi_own, own_cols], got_up.at[1], b + 1, p), has_u),
        (send(5, has_d, mask.at[hi8], mask_up, b + 1, p), has_u),
        (send(6, has_l, ledge, got_r, b, p - 1), has_r),
        (send(7, has_r, redge, got_l, b, p + 1), has_l),
        (send(8, has_d & has_r, redge.at[hi8], corner.at[0], b + 1, p + 1), has_u & has_l),
        (send(9, has_d & has_l, ledge.at[hi8], corner.at[1], b + 1, p - 1), has_u & has_r),
        (send(10, has_u & has_r, redge.at[lo8], corner.at[2], b - 1, p + 1), has_d & has_l),
        (send(11, has_u & has_l, ledge.at[lo8], corner.at[3], b - 1, p - 1), has_d & has_r),
    )
    for (there, copy), _ in halos:
        pl.when(there)(copy.start)

    def blank(flag, ref):
        @pl.when(jnp.logical_not(flag))
        def _():
            ref[...] = jnp.zeros(ref.shape, ref.dtype)

    blank(has_d, got_dn)
    blank(has_d, mask_dn)
    blank(has_u, got_up)
    blank(has_u, mask_up)
    blank(has_r, got_r)
    blank(has_l, got_l)
    blank(has_u & has_l, corner.at[0])
    blank(has_u & has_r, corner.at[1])
    blank(has_d & has_l, corner.at[2])
    blank(has_d & has_r, corner.at[3])

    lax.fori_loop(EARLY, PANELS // 128, turn, 0)

    for (there, copy), comes in halos:
        pl.when(comes)(copy.wait_recv)
        pl.when(there)(copy.wait_send)

    def side(left, right, shift, lane):
        return jnp.where(
            lane < 4, roll(right, -shift, 1), jnp.where(lane >= 124, roll(left, shift, 1), 0.0)
        )

    gl, gr = got_l[...], got_r[...]
    ea[FIRST:BOT, COLS:] = side(gl, gr, 0, lane)
    ev[FIRST:BOT, COLS:] = side(gl, gr, 4, lane)
    em[FIRST:BOT, COLS:] = side(gl, gr, 8, lane)
    lane8 = lax.broadcasted_iota(jnp.int32, (8, 128), 1)
    sub8 = lax.broadcasted_iota(jnp.int32, (8, 128), 0)
    sub_w = lax.broadcasted_iota(jnp.int32, (8, COLS), 0)
    for start, keep, keep_w, got, gmask, cl, cr in (
        (TOP, sub8 >= 4, sub_w >= 4, got_up, mask_up, corner[0], corner[1]),
        (BOT, sub8 < 4, sub_w < 4, got_dn, mask_dn, corner[2], corner[3]),
    ):
        rows = pl.ds(start, 8)
        ea[rows, :COLS] = jnp.where(keep_w, got[0], 0.0)
        ev[rows, :COLS] = jnp.where(keep_w, got[1], 0.0)
        em[rows, :COLS] = jnp.where(keep_w, gmask[...].astype(jnp.float32), 0.0)
        ea[rows, COLS:] = jnp.where(keep, side(cl, cr, 0, lane8), 0.0)
        ev[rows, COLS:] = jnp.where(keep, side(cl, cr, 4, lane8), 0.0)
        em[rows, COLS:] = jnp.where(keep, side(cl, cr, 8, lane8), 0.0)

    crow = cell[...] >> 9
    ccol = cell[...] & (COLS - 1)
    pick_c = jnp.where(
        lax.broadcasted_iota(jnp.int32, (COLS, OWN), 0) == ccol, 1.0, 0.0
    ).astype(jnp.bfloat16)
    pick_r = lax.broadcasted_iota(jnp.int32, (ROWS, OWN), 0) == crow
    for step in range(STEPS):
        src, dst = (ea, eb) if step % 2 == 0 else (eb, ea)

        def advance(i, _, src=src, dst=dst):
            at = pl.multiple_of(TOP + STRIP * i, 8)
            rows = pl.ds(at, STRIP)
            wide = src[pl.ds(pl.multiple_of(at - 8, 8), STRIP + 16), :]
            center = wide[8 : STRIP + 8]
            west = roll(wide, 1, 0)[8 : STRIP + 8]
            east = roll(wide, -1, 0)[8 : STRIP + 8]
            south = roll(center, 1, 1)
            north = roll(center, -1, 1)
            dx, dy = east - west, north - south
            square = dx * dx + dy * dy
            h = square * lax.rsqrt(jnp.maximum(square, 1e-30))
            viscosity = ev[rows, :] + 0.05 * h / (2.0 + h)
            spread = (east + west) + (north + south) - 4.0 * center
            update = 0.75 * center + 0.15 * west + 0.1 * south + viscosity * spread
            dst[rows, :] = em[rows, :] * update
            return 0

        lax.fori_loop(0, (EXT_R - 16) // STRIP, advance, 0)
        found = jnp.dot(
            dst[FIRST:BOT, :COLS].astype(jnp.bfloat16), pick_c, preferred_element_type=jnp.float32
        )
        samp_own[step : step + 1, :] = jnp.sum(jnp.where(pick_r, found, 0.0), axis=0, keepdims=True)

    out = pltpu.make_async_copy(ea.at[own_rows, own_cols], field_out, store)
    out.start()

    mine = pl.ds(pl.multiple_of(p * OWN, OWN), OWN)
    samp_all[:, mine] = samp_own[...]

    def samp_copy(k):
        to = lax.rem(p + k, PAN)
        return pltpu.make_async_remote_copy(
            src_ref=samp_own, dst_ref=samp_all.at[:, mine], send_sem=samp_send.at[k],
            recv_sem=samp_recv.at[p], device_id=(b, to), device_id_type=MESH,
        )

    def samp_arrival(k):
        frm = lax.rem(p + k, PAN)
        return pltpu.make_async_remote_copy(
            src_ref=samp_own, dst_ref=samp_all.at[:, pl.ds(pl.multiple_of(frm * OWN, OWN), OWN)],
            send_sem=samp_send.at[k], recv_sem=samp_recv.at[frm], device_id=(b, frm), device_id_type=MESH,
        )

    for k in range(1, PAN):
        samp_copy(k).start()
    for k in range(1, PAN):
        samp_arrival(k).wait_recv()
    for t in range(STEPS):
        sb[t] = jnp.broadcast_to(samp_all[t : t + 1, :], (16, PANELS)).astype(jnp.bfloat16)

    io16 = lax.broadcasted_iota(jnp.int32, (16, KT), 0).astype(jnp.float32)
    lane16 = lax.broadcasted_iota(jnp.int32, (16, 128), 1)
    sub16 = lax.broadcasted_iota(jnp.int32, (16, 128), 0)
    zero = jnp.zeros((16, KT), jnp.bfloat16)

    def bin_group(first, slot):
        acc = None
        for k in range(PANELS // KT):
            ks = pl.ds(k * KT, KT)
            ss = [sb[t, :, ks] for t in range(STEPS)]
            lhs, rhs = [], []
            for i in range(STACK):
                o = pl.ds(first + i, 1)
                hb = jnp.broadcast_to(high_t[o, ks], (16, KT)).astype(jnp.bfloat16)
                ab = jnp.broadcast_to(amp_t[o, ks], (16, KT)).astype(jnp.bfloat16)
                lb = jnp.broadcast_to(low_t[o, ks], (16, KT)).astype(jnp.bfloat16)
                for j in range(HIGH // 16):
                    lhs.append(jnp.where(hb == (io16 + 16 * j).astype(jnp.bfloat16), ab, zero))
                for j in range(LOW // 16):
                    v = zero
                    for t in range(STEPS):
                        v = jnp.where(lb == (io16 + (16 * j - t)).astype(jnp.bfloat16), ss[t], v)
                    rhs.append(v)
            part = lax.dot_general(
                jnp.concatenate(lhs, 0), jnp.concatenate(rhs, 0), (((1,), (1,)), ((), ())),
                preferred_element_type=jnp.float32,
            )
            acc = part if acc is None else acc + part
        for i in range(STACK):
            total = None
            for r in range(PARTS):
                blk = acc[i * HIGH + 16 * r : i * HIGH + 16 * r + 16, :]
                blk = jnp.where((lane16 >= LOW * i) & (lane16 < LOW * i + LOW), blk, 0.0)
                if (RADIX * r - LOW * i) % 128:
                    blk = roll(blk, RADIX * r - LOW * i, 1)
                if r == PARTS - 1:
                    over = jnp.where((lane16 < 8) & (sub16 < 15), blk, 0.0)
                    blk = jnp.where(lane16 < 8, 0.0, blk) + roll(over, 1, 0)
                total = blk if total is None else total + blk
            hist[pl.ds(slot + i, 16, stride=PITCH), :] = total

    def bin_copy(k, h):
        to = lax.rem(b + k, BOX)
        rows = pl.ds(pl.multiple_of(h * HALF, HALF), HALF)
        return pltpu.make_async_remote_copy(
            src_ref=outbox.at[to, rows], dst_ref=inbox.at[b, rows], send_sem=bin_send.at[k],
            recv_sem=bin_recv.at[b], device_id=(to, p), device_id_type=MESH,
        )

    def bin_whole(k):
        frm = lax.rem(b + k, BOX)
        return pltpu.make_async_remote_copy(
            src_ref=outbox.at[frm], dst_ref=inbox.at[frm], send_sem=bin_send.at[k],
            recv_sem=bin_recv.at[frm], device_id=(frm, p), device_id_type=MESH,
        )

    def scale_copy(k):
        to = lax.rem(b + k, BOX)
        return pltpu.make_async_remote_copy(
            src_ref=scale_out.at[to], dst_ref=inscales.at[b], send_sem=sc_send.at[k],
            recv_sem=sc_recv.at[b], device_id=(to, p), device_id_type=MESH,
        )

    def scale_arrival(k):
        frm = lax.rem(b + k, BOX)
        return pltpu.make_async_remote_copy(
            src_ref=scale_out.at[frm], dst_ref=inscales.at[frm], send_sem=sc_send.at[k],
            recv_sem=sc_recv.at[frm], device_id=(frm, p), device_id_type=MESH,
        )

    def pack(h, part):
        rows = pl.ds(pl.multiple_of(h * HALF, HALF), HALF)
        for q in range(BOX):
            at = q * PITCH + part * HALF
            x = hist[at : at + HALF, :]
            most = jnp.max(jnp.max(jnp.abs(x), axis=0, keepdims=True), axis=1, keepdims=True)
            most = jnp.maximum(jnp.broadcast_to(most, (1, 128)), 1e-30)
            unit = (most * (1.0 / TOPINT)).astype(jnp.bfloat16).astype(jnp.float32)
            y = jnp.floor(x * (1.0 / unit) + 0.5)
            outbox[q, rows, :] = y.astype(jnp.int32).astype(jnp.int16)
            scales[q, pl.ds(h, 1), :] = unit

    def post(h):
        for k in ORDER:
            bin_copy(k, h).start()

    def chunk(c, _):
        before = jnp.maximum(2 * c - 1, 1)
        pack(before, 1)
        for u in range(HALF // STACK):
            bin_group(c * CHUNK + u * STACK, u * STACK)
        pack(2 * c, 0)
        for u in range(HALF // STACK, CHUNK // STACK):
            bin_group(c * CHUNK + u * STACK, u * STACK)

        @pl.when(c > 0)
        def _():
            post(before)

        post(2 * c)
        return 0

    lax.fori_loop(0, CHUNKS, chunk, 0)
    pack(HALVES - 1, 1)
    post(HALVES - 1)
    scale_out[...] = scales[...].astype(jnp.bfloat16)
    for k in ORDER:
        scale_copy(k).start()
    inscales[b] = scale_out[b]
    inbox[b] = outbox[b]

    def arrive(k, _):
        scale_arrival(k).wait_recv()
        bin_whole(k).wait_recv()
        return 0

    lax.fori_loop(1, BOX, arrive, 0)

    for s in range(BOX):
        units[s] = inscales[s].astype(jnp.float32)

    def gather(h, _):
        rows = pl.ds(pl.multiple_of(h * HALF, HALF), HALF)
        total = None
        for s in range(BOX):
            x = inbox[s, rows, :].astype(jnp.int32).astype(jnp.float32) * units[s, pl.ds(h, 1), :]
            total = x if total is None else total + x
        sig_out[rows, :] = total
        return 0

    lax.fori_loop(0, HALVES, gather, 0)

    out.wait()
    for k in range(1, PAN):
        samp_copy(k).wait_send()

    def sent(k, _):
        scale_copy(k).wait_send()
        bin_whole(k).wait_send()
        return 0

    lax.fori_loop(1, BOX, sent, 0)


def hand_over(field, signals, field_out, sig_out, sems):
    copies = (
        pltpu.make_async_copy(field, field_out, sems.at[0]),
        pltpu.make_async_copy(signals, sig_out, sems.at[1]),
    )
    for copy in copies:
        copy.start()
    for copy in copies:
        copy.wait()


def on_device(field_start, fluid_mask, base_visc, panel_cell, amplitude, delay_bin):
    f32, bf16, i32 = jnp.float32, jnp.bfloat16, jnp.int32
    vmem = lambda shape, dtype=f32: pltpu.VMEM(shape, dtype)
    dma = lambda *shape: pltpu.SemaphoreType.DMA(shape)
    scratch = [
        vmem((ROWS, COLS), i32), vmem((1, OWN), i32), vmem((PANELS, OBS), bf16), vmem((PANELS, OBS), i32),
        vmem((EXT_R, EXT_C)), vmem((EXT_R, EXT_C)), vmem((EXT_R, EXT_C)), vmem((EXT_R, EXT_C)),
        vmem((ROWS, 128)), vmem((ROWS, 128)),
        vmem((2, 8, COLS)), vmem((2, 8, COLS)), vmem((8, COLS), i32), vmem((8, COLS), i32),
        vmem((ROWS, 128)), vmem((ROWS, 128)), vmem((4, 8, 128)),
        vmem((8, OWN)), vmem((8, PANELS)),
        vmem((OBS, PANELS)), vmem((OBS, PANELS)), vmem((OBS, PANELS)),
        vmem((STEPS, 16, PANELS), bf16),
        vmem((BOX * PITCH, 128)),
        vmem((BOX, OBS, 128), jnp.int16), vmem((BOX, HALVES, 128)), vmem((BOX, HALVES, 128), bf16),
        vmem((BOX, OBS, 128), jnp.int16), vmem((BOX, HALVES, 128), bf16), vmem((BOX, HALVES, 128)),
        dma(6), pltpu.SemaphoreType.DMA, dma(12), dma(12), dma(PAN), dma(PAN), dma(BOX), dma(BOX), dma(BOX), dma(BOX),
    ]
    field, signals = pl.pallas_call(
        kernel,
        out_shape=(
            jax.ShapeDtypeStruct((ROWS, COLS), f32),
            jax.ShapeDtypeStruct((OBS, NB // BOX), f32),
        ),
        in_specs=[pl.BlockSpec(memory_space=pl.ANY)] * 6,
        out_specs=(pl.BlockSpec(memory_space=pl.ANY), pl.BlockSpec(memory_space=pltpu.VMEM)),
        scratch_shapes=scratch,
        compiler_params=pltpu.CompilerParams(
            collective_id=0, has_side_effects=True, vmem_limit_bytes=56 * 2**20
        ),
    )(field_start, fluid_mask, base_visc, panel_cell.reshape(1, OWN), amplitude, delay_bin)
    return pl.pallas_call(
        hand_over,
        out_shape=(
            jax.ShapeDtypeStruct((ROWS, COLS), f32),
            jax.ShapeDtypeStruct((OBS, NB // BOX), f32),
        ),
        in_specs=[pl.BlockSpec(memory_space=pltpu.VMEM)] * 2,
        out_specs=(pl.BlockSpec(memory_space=pl.ANY),) * 2,
        scratch_shapes=[dma(2)],
        compiler_params=pltpu.CompilerParams(vmem_limit_bytes=4 * 2**20),
    )(field, signals)


def solution(mesh):
    placed = (
        P("box", "panel"),
        P("box", "panel"),
        P("box", "panel"),
        P(("box", "panel")),
        P("box", "panel"),
        P("box", "panel"),
    )
    return jax.shard_map(
        on_device,
        mesh=mesh,
        in_specs=placed,
        out_specs=(P("box", "panel"), P("panel", "box")),
        check_vma=False,
    )
```

```python
import functools

import jax
import jax.numpy as jnp
from jax import lax
from jax.experimental import pallas as pl
from jax.experimental.pallas import tpu as pltpu
from jax.sharding import PartitionSpec as P

MESH = pl.DeviceIdType.MESH
STEPS = 4
NB = 2048
BOX = 16
PAN = 8
ROWS, COLS = 256, 512
PANELS, OBS, OWN = 1024, 512, 128
TOP, FIRST, BOT, EXT_R, EXT_C = 8, 16, 272, 304, 640
STRIP = 96
RADIX, PARTS, HIGH, LOW = 26, 5, 80, 32
STACK = 4
KT = 256
EARLY = 3
CHUNK = 64
CHUNKS = OBS // CHUNK
HALF = CHUNK // 2
HALVES = OBS // HALF
PITCH = CHUNK + 8
TOPINT = 32000.0
ORDER = (10, 9, 11, 6, 14, 8, 2, 5, 7, 13, 15, 12, 4, 3, 1)


def roll(x, shift, axis):
    return pltpu.roll(x, shift % x.shape[axis], axis)


def kernel(
    field_in, mask_in, visc_in, cell_in, amp_in, dly_in, field_out, sig_out,
    mask, cell, amp, dly, ea, eb, em, ev, ledge, redge, got_up, got_dn, mask_up, mask_dn, got_l, got_r, corner,
    samp_own, samp_all, amp_t, high_t, low_t, sb, hist, outbox, scales, scale_out, inbox, inscales, units,
    loads, store, halo_send, halo_recv, samp_send, samp_recv, bin_send, bin_recv, sc_send, sc_recv,
):
    b = lax.axis_index("box")
    p = lax.axis_index("panel")
    has_u, has_d, has_l, has_r = b > 0, b < BOX - 1, p > 0, p < PAN - 1
    diagonals = (
        (has_u & has_l, b - 1, p - 1),
        (has_u & has_r, b - 1, p + 1),
        (has_d & has_l, b + 1, p - 1),
        (has_d & has_r, b + 1, p + 1),
    )

    own_rows, own_cols = pl.ds(FIRST, ROWS), pl.ds(0, COLS)
    arrivals = [
        pltpu.make_async_copy(src, dst, loads.at[i])
        for i, (src, dst) in enumerate((
            (field_in, ea.at[own_rows, own_cols]), (visc_in, ev.at[own_rows, own_cols]),
            (mask_in, mask), (cell_in, cell), (amp_in, amp), (dly_in, dly),
        ))
    ]
    for copy in arrivals:
        copy.start()

    barrier = pltpu.get_barrier_semaphore()

    def greet(bb, pp):
        pl.semaphore_signal(barrier, inc=1, device_id=(bb, pp), device_id_type=MESH)

    for k in range(1, PAN):
        greet(b, lax.rem(p + k, PAN))
    for k in range(1, BOX):
        greet(lax.rem(b + k, BOX), p)
    expected = jnp.int32(PAN - 1 + BOX - 1)
    for there, bb, pp in diagonals:
        expected = expected + there.astype(jnp.int32)

        @pl.when(there)
        def _(bb=bb, pp=pp):
            greet(bb, pp)

    for buf in (ea, eb, ev, em):
        buf[0:8, :] = jnp.zeros((8, EXT_C), jnp.float32)
        buf[BOT + 8 :, :] = jnp.zeros((EXT_R - BOT - 8, EXT_C), jnp.float32)
    hist[...] = jnp.zeros_like(hist)
    samp_own[...] = jnp.zeros_like(samp_own)
    for copy in arrivals[:4]:
        copy.wait()

    lane = lax.broadcasted_iota(jnp.int32, (ROWS, 128), 1)
    fe, ve = ea[own_rows, :128], ev[own_rows, :128]
    me = mask[:, :128].astype(jnp.float32)
    ledge[...] = jnp.where(
        lane < 4, fe, jnp.where(lane < 8, roll(ve, 4, 1), jnp.where(lane < 12, roll(me, 8, 1), 0.0))
    )
    fe, ve = ea[own_rows, COLS - 128 : COLS], ev[own_rows, COLS - 128 : COLS]
    me = mask[:, COLS - 128 :].astype(jnp.float32)
    redge[...] = jnp.where(
        lane >= 124, fe, jnp.where(lane >= 120, roll(ve, -4, 1), jnp.where(lane >= 116, roll(me, -8, 1), 0.0))
    )
    em[own_rows, :COLS] = mask[...].astype(jnp.float32)
    for copy in arrivals[4:]:
        copy.wait()

    def turn(i, _):
        ps = pl.ds(pl.multiple_of(i * 128, 128), 128)
        for c in range(OBS // 128):
            cs = pl.ds(c * 128, 128)
            amp_t[cs, ps] = amp[ps, cs].astype(jnp.float32).T
            d = dly[ps, cs]
            low = d & 127
            r = (low * 79) >> 11
            high_t[cs, ps] = (r * 16 + (d >> 7)).astype(jnp.float32).T
            low_t[cs, ps] = (low - RADIX * r).astype(jnp.float32).T
        return 0

    lax.fori_loop(0, EARLY, turn, 0)

    def send(i, there, src, dst, bb, pp):
        copy = pltpu.make_async_remote_copy(
            src_ref=src, dst_ref=dst, send_sem=halo_send.at[i], recv_sem=halo_recv.at[i],
            device_id=(bb, pp), device_id_type=MESH,
        )
        return there, copy

    pl.semaphore_wait(barrier, expected)

    lo8, hi8 = pl.ds(0, 8), pl.ds(ROWS - 8, 8)
    lo_own, hi_own = pl.ds(FIRST, 8), pl.ds(BOT - 8, 8)
    halos = (
        (send(0, has_u, ea.at[lo_own, own_cols], got_dn.at[0], b - 1, p), has_d),
        (send(1, has_u, ev.at[lo_own, own_cols], got_dn.at[1], b - 1, p), has_d),
        (send(2, has_u, mask.at[lo8], mask_dn, b - 1, p), has_d),
        (send(3, has_d, ea.at[hi_own, own_cols], got_up.at[0], b + 1, p), has_u),
        (send(4, has_d, ev.at[hi_own, own_cols], got_up.at[1], b + 1, p), has_u),
        (send(5, has_d, mask.at[hi8], mask_up, b + 1, p), has_u),
        (send(6, has_l, ledge, got_r, b, p - 1), has_r),
        (send(7, has_r, redge, got_l, b, p + 1), has_l),
        (send(8, has_d & has_r, redge.at[hi8], corner.at[0], b + 1, p + 1), has_u & has_l),
        (send(9, has_d & has_l, ledge.at[hi8], corner.at[1], b + 1, p - 1), has_u & has_r),
        (send(10, has_u & has_r, redge.at[lo8], corner.at[2], b - 1, p + 1), has_d & has_l),
        (send(11, has_u & has_l, ledge.at[lo8], corner.at[3], b - 1, p - 1), has_d & has_r),
    )
    for (there, copy), _ in halos:
        pl.when(there)(copy.start)

    def blank(flag, ref):
        @pl.when(jnp.logical_not(flag))
        def _():
            ref[...] = jnp.zeros(ref.shape, ref.dtype)

    blank(has_d, got_dn)
    blank(has_d, mask_dn)
    blank(has_u, got_up)
    blank(has_u, mask_up)
    blank(has_r, got_r)
    blank(has_l, got_l)
    blank(has_u & has_l, corner.at[0])
    blank(has_u & has_r, corner.at[1])
    blank(has_d & has_l, corner.at[2])
    blank(has_d & has_r, corner.at[3])

    lax.fori_loop(EARLY, PANELS // 128, turn, 0)

    for (there, copy), comes in halos:
        pl.when(comes)(copy.wait_recv)
        pl.when(there)(copy.wait_send)

    def side(left, right, shift, lane):
        return jnp.where(
            lane < 4, roll(right, -shift, 1), jnp.where(lane >= 124, roll(left, shift, 1), 0.0)
        )

    gl, gr = got_l[...], got_r[...]
    ea[FIRST:BOT, COLS:] = side(gl, gr, 0, lane)
    ev[FIRST:BOT, COLS:] = side(gl, gr, 4, lane)
    em[FIRST:BOT, COLS:] = side(gl, gr, 8, lane)
    lane8 = lax.broadcasted_iota(jnp.int32, (8, 128), 1)
    sub8 = lax.broadcasted_iota(jnp.int32, (8, 128), 0)
    sub_w = lax.broadcasted_iota(jnp.int32, (8, COLS), 0)
    for start, keep, keep_w, got, gmask, cl, cr in (
        (TOP, sub8 >= 4, sub_w >= 4, got_up, mask_up, corner[0], corner[1]),
        (BOT, sub8 < 4, sub_w < 4, got_dn, mask_dn, corner[2], corner[3]),
    ):
        rows = pl.ds(start, 8)
        ea[rows, :COLS] = jnp.where(keep_w, got[0], 0.0)
        ev[rows, :COLS] = jnp.where(keep_w, got[1], 0.0)
        em[rows, :COLS] = jnp.where(keep_w, gmask[...].astype(jnp.float32), 0.0)
        ea[rows, COLS:] = jnp.where(keep, side(cl, cr, 0, lane8), 0.0)
        ev[rows, COLS:] = jnp.where(keep, side(cl, cr, 4, lane8), 0.0)
        em[rows, COLS:] = jnp.where(keep, side(cl, cr, 8, lane8), 0.0)

    crow = cell[...] >> 9
    ccol = cell[...] & (COLS - 1)
    pick_c = jnp.where(
        lax.broadcasted_iota(jnp.int32, (COLS, OWN), 0) == ccol, 1.0, 0.0
    ).astype(jnp.bfloat16)
    pick_r = lax.broadcasted_iota(jnp.int32, (ROWS, OWN), 0) == crow
    for step in range(STEPS):
        src, dst = (ea, eb) if step % 2 == 0 else (eb, ea)

        def advance(i, _, src=src, dst=dst):
            at = pl.multiple_of(TOP + STRIP * i, 8)
            rows = pl.ds(at, STRIP)
            wide = src[pl.ds(pl.multiple_of(at - 8, 8), STRIP + 16), :]
            center = wide[8 : STRIP + 8]
            west = roll(wide, 1, 0)[8 : STRIP + 8]
            east = roll(wide, -1, 0)[8 : STRIP + 8]
            south = roll(center, 1, 1)
            north = roll(center, -1, 1)
            dx, dy = east - west, north - south
            square = dx * dx + dy * dy
            h = square * lax.rsqrt(jnp.maximum(square, 1e-30))
            viscosity = ev[rows, :] + 0.05 * h / (2.0 + h)
            spread = (east + west) + (north + south) - 4.0 * center
            update = 0.75 * center + 0.15 * west + 0.1 * south + viscosity * spread
            dst[rows, :] = em[rows, :] * update
            return 0

        lax.fori_loop(0, (EXT_R - 16) // STRIP, advance, 0)
        found = jnp.dot(
            dst[FIRST:BOT, :COLS].astype(jnp.bfloat16), pick_c, preferred_element_type=jnp.float32
        )
        samp_own[step : step + 1, :] = jnp.sum(jnp.where(pick_r, found, 0.0), axis=0, keepdims=True)

    out = pltpu.make_async_copy(ea.at[own_rows, own_cols], field_out, store)
    out.start()

    mine = pl.ds(pl.multiple_of(p * OWN, OWN), OWN)
    samp_all[:, mine] = samp_own[...]

    def samp_copy(k):
        to = lax.rem(p + k, PAN)
        return pltpu.make_async_remote_copy(
            src_ref=samp_own, dst_ref=samp_all.at[:, mine], send_sem=samp_send.at[k],
            recv_sem=samp_recv.at[p], device_id=(b, to), device_id_type=MESH,
        )

    def samp_arrival(k):
        frm = lax.rem(p + k, PAN)
        return pltpu.make_async_remote_copy(
            src_ref=samp_own, dst_ref=samp_all.at[:, pl.ds(pl.multiple_of(frm * OWN, OWN), OWN)],
            send_sem=samp_send.at[k], recv_sem=samp_recv.at[frm], device_id=(b, frm), device_id_type=MESH,
        )

    for k in range(1, PAN):
        samp_copy(k).start()
    for k in range(1, PAN):
        samp_arrival(k).wait_recv()
    for t in range(STEPS):
        sb[t] = jnp.broadcast_to(samp_all[t : t + 1, :], (16, PANELS)).astype(jnp.bfloat16)

    io16 = lax.broadcasted_iota(jnp.int32, (16, KT), 0).astype(jnp.float32)
    lane16 = lax.broadcasted_iota(jnp.int32, (16, 128), 1)
    sub16 = lax.broadcasted_iota(jnp.int32, (16, 128), 0)
    zero = jnp.zeros((16, KT), jnp.bfloat16)

    def bin_group(first, slot):
        acc = None
        for k in range(PANELS // KT):
            ks = pl.ds(k * KT, KT)
            ss = [sb[t, :, ks] for t in range(STEPS)]
            lhs, rhs = [], []
            for i in range(STACK):
                o = pl.ds(first + i, 1)
                hb = jnp.broadcast_to(high_t[o, ks], (16, KT)).astype(jnp.bfloat16)
                ab = jnp.broadcast_to(amp_t[o, ks], (16, KT)).astype(jnp.bfloat16)
                lb = jnp.broadcast_to(low_t[o, ks], (16, KT)).astype(jnp.bfloat16)
                for j in range(HIGH // 16):
                    lhs.append(jnp.where(hb == (io16 + 16 * j).astype(jnp.bfloat16), ab, zero))
                for j in range(LOW // 16):
                    v = zero
                    for t in range(STEPS):
                        v = jnp.where(lb == (io16 + (16 * j - t)).astype(jnp.bfloat16), ss[t], v)
                    rhs.append(v)
            part = lax.dot_general(
                jnp.concatenate(lhs, 0), jnp.concatenate(rhs, 0), (((1,), (1,)), ((), ())),
                preferred_element_type=jnp.float32,
            )
            acc = part if acc is None else acc + part
        for i in range(STACK):
            total = None
            for r in range(PARTS):
                blk = acc[i * HIGH + 16 * r : i * HIGH + 16 * r + 16, :]
                blk = jnp.where((lane16 >= LOW * i) & (lane16 < LOW * i + LOW), blk, 0.0)
                if (RADIX * r - LOW * i) % 128:
                    blk = roll(blk, RADIX * r - LOW * i, 1)
                if r == PARTS - 1:
                    over = jnp.where((lane16 < 8) & (sub16 < 15), blk, 0.0)
                    blk = jnp.where(lane16 < 8, 0.0, blk) + roll(over, 1, 0)
                total = blk if total is None else total + blk
            hist[pl.ds(slot + i, 16, stride=PITCH), :] = total

    def bin_copy(k, h):
        to = lax.rem(b + k, BOX)
        rows = pl.ds(pl.multiple_of(h * HALF, HALF), HALF)
        return pltpu.make_async_remote_copy(
            src_ref=outbox.at[to, rows], dst_ref=inbox.at[b, rows], send_sem=bin_send.at[k],
            recv_sem=bin_recv.at[b], device_id=(to, p), device_id_type=MESH,
        )

    def bin_whole(k):
        frm = lax.rem(b + k, BOX)
        return pltpu.make_async_remote_copy(
            src_ref=outbox.at[frm], dst_ref=inbox.at[frm], send_sem=bin_send.at[k],
            recv_sem=bin_recv.at[frm], device_id=(frm, p), device_id_type=MESH,
        )

    def scale_copy(k):
        to = lax.rem(b + k, BOX)
        return pltpu.make_async_remote_copy(
            src_ref=scale_out.at[to], dst_ref=inscales.at[b], send_sem=sc_send.at[k],
            recv_sem=sc_recv.at[b], device_id=(to, p), device_id_type=MESH,
        )

    def scale_arrival(k):
        frm = lax.rem(b + k, BOX)
        return pltpu.make_async_remote_copy(
            src_ref=scale_out.at[frm], dst_ref=inscales.at[frm], send_sem=sc_send.at[k],
            recv_sem=sc_recv.at[frm], device_id=(frm, p), device_id_type=MESH,
        )

    def pack(h, part):
        rows = pl.ds(pl.multiple_of(h * HALF, HALF), HALF)
        for q in range(BOX):
            at = q * PITCH + part * HALF
            x = hist[at : at + HALF, :]
            most = jnp.max(jnp.max(jnp.abs(x), axis=0, keepdims=True), axis=1, keepdims=True)
            most = jnp.maximum(jnp.broadcast_to(most, (1, 128)), 1e-30)
            unit = (most * (1.0 / TOPINT)).astype(jnp.bfloat16).astype(jnp.float32)
            y = jnp.floor(x * (1.0 / unit) + 0.5)
            outbox[q, rows, :] = y.astype(jnp.int32).astype(jnp.int16)
            scales[q, pl.ds(h, 1), :] = unit

    def post(h):
        for k in ORDER:
            bin_copy(k, h).start()

    def chunk(c, _):
        before = jnp.maximum(2 * c - 1, 1)
        pack(before, 1)
        for u in range(HALF // STACK):
            bin_group(c * CHUNK + u * STACK, u * STACK)
        pack(2 * c, 0)
        for u in range(HALF // STACK, CHUNK // STACK):
            bin_group(c * CHUNK + u * STACK, u * STACK)

        @pl.when(c > 0)
        def _():
            post(before)

        post(2 * c)
        return 0

    lax.fori_loop(0, CHUNKS, chunk, 0)
    pack(HALVES - 1, 1)
    post(HALVES - 1)
    scale_out[...] = scales[...].astype(jnp.bfloat16)
    for k in ORDER:
        scale_copy(k).start()
    inscales[b] = scale_out[b]
    inbox[b] = outbox[b]

    def arrive(k, _):
        scale_arrival(k).wait_recv()
        bin_whole(k).wait_recv()
        return 0

    lax.fori_loop(1, BOX, arrive, 0)

    for s in range(BOX):
        units[s] = inscales[s].astype(jnp.float32)

    def gather(h, _):
        rows = pl.ds(pl.multiple_of(h * HALF, HALF), HALF)
        total = None
        for s in range(BOX):
            x = inbox[s, rows, :].astype(jnp.int32).astype(jnp.float32) * units[s, pl.ds(h, 1), :]
            total = x if total is None else total + x
        sig_out[rows, :] = total
        return 0

    lax.fori_loop(0, HALVES, gather, 0)

    out.wait()
    for k in range(1, PAN):
        samp_copy(k).wait_send()

    def sent(k, _):
        scale_copy(k).wait_send()
        bin_whole(k).wait_send()
        return 0

    lax.fori_loop(1, BOX, sent, 0)


def hand_over(field, signals, field_out, sig_out, sems):
    copies = (
        pltpu.make_async_copy(field, field_out, sems.at[0]),
        pltpu.make_async_copy(signals, sig_out, sems.at[1]),
    )
    for copy in copies:
        copy.start()
    for copy in copies:
        copy.wait()


def on_device(field_start, fluid_mask, base_visc, panel_cell, amplitude, delay_bin):
    f32, bf16, i32 = jnp.float32, jnp.bfloat16, jnp.int32
    vmem = lambda shape, dtype=f32: pltpu.VMEM(shape, dtype)
    dma = lambda *shape: pltpu.SemaphoreType.DMA(shape)
    scratch = [
        vmem((ROWS, COLS), i32), vmem((1, OWN), i32), vmem((PANELS, OBS), bf16), vmem((PANELS, OBS), i32),
        vmem((EXT_R, EXT_C)), vmem((EXT_R, EXT_C)), vmem((EXT_R, EXT_C)), vmem((EXT_R, EXT_C)),
        vmem((ROWS, 128)), vmem((ROWS, 128)),
        vmem((2, 8, COLS)), vmem((2, 8, COLS)), vmem((8, COLS), i32), vmem((8, COLS), i32),
        vmem((ROWS, 128)), vmem((ROWS, 128)), vmem((4, 8, 128)),
        vmem((8, OWN)), vmem((8, PANELS)),
        vmem((OBS, PANELS)), vmem((OBS, PANELS)), vmem((OBS, PANELS)),
        vmem((STEPS, 16, PANELS), bf16),
        vmem((BOX * PITCH, 128)),
        vmem((BOX, OBS, 128), jnp.int16), vmem((BOX, HALVES, 128)), vmem((BOX, HALVES, 128), bf16),
        vmem((BOX, OBS, 128), jnp.int16), vmem((BOX, HALVES, 128), bf16), vmem((BOX, HALVES, 128)),
        dma(6), pltpu.SemaphoreType.DMA, dma(12), dma(12), dma(PAN), dma(PAN), dma(BOX), dma(BOX), dma(BOX), dma(BOX),
    ]
    field, signals = pl.pallas_call(
        kernel,
        out_shape=(
            pltpu.VMEM((ROWS, COLS), f32),
            pltpu.VMEM((OBS, NB // BOX), f32),
        ),
        in_specs=[pl.BlockSpec(memory_space=pl.ANY)] * 6,
        out_specs=(pl.BlockSpec(memory_space=pl.ANY), pl.BlockSpec(memory_space=pltpu.VMEM)),
        scratch_shapes=scratch,
        compiler_params=pltpu.CompilerParams(
            collective_id=0, has_side_effects=True, vmem_limit_bytes=56 * 2**20
        ),
    )(field_start, fluid_mask, base_visc, panel_cell.reshape(1, OWN), amplitude, delay_bin)
    return pl.pallas_call(
        hand_over,
        out_shape=(
            jax.ShapeDtypeStruct((ROWS, COLS), f32),
            jax.ShapeDtypeStruct((OBS, NB // BOX), f32),
        ),
        in_specs=[pl.BlockSpec(memory_space=pltpu.VMEM)] * 2,
        out_specs=(pl.BlockSpec(memory_space=pl.ANY),) * 2,
        scratch_shapes=[dma(2)],
        compiler_params=pltpu.CompilerParams(vmem_limit_bytes=4 * 2**20),
    )(field, signals)


def solution(mesh):
    placed = (
        P("box", "panel"),
        P("box", "panel"),
        P("box", "panel"),
        P(("box", "panel")),
        P("box", "panel"),
        P("box", "panel"),
    )
    return jax.shard_map(
        on_device,
        mesh=mesh,
        in_specs=placed,
        out_specs=(P("box", "panel"), P("panel", "box")),
        check_vma=False,
    )
```

```python
import functools

import jax
import jax.numpy as jnp
from jax import lax
from jax.experimental import pallas as pl
from jax.experimental.pallas import tpu as pltpu
from jax.sharding import PartitionSpec as P

MESH = pl.DeviceIdType.MESH
STEPS = 4
NB = 2048
BOX = 16
SIDE = 4
PAN = 8
ROWS, COLS = 256, 512
PANELS, OBS, OWN = 1024, 512, 128
TOP, FIRST, BOT, EXT_R, EXT_C = 8, 16, 272, 304, 640
STRIP = 96
RADIX, PARTS, HIGH, LOW = 26, 5, 80, 32
STACK = 4
KT = 256
EARLY = 3
CHUNK = 64
CHUNKS = OBS // CHUNK
HALF = CHUNK // 2
HALVES = OBS // HALF
PITCH = CHUNK + 8
TOPINT = 32000.0
ORDER = (10, 9, 11, 6, 14, 8, 2, 5, 7, 13, 15, 12, 4, 3, 1)


def roll(x, shift, axis):
    return pltpu.roll(x, shift % x.shape[axis], axis)


def kernel(
    field_in, mask_in, visc_in, cell_in, amp_in, dly_in, field_out, sig_out,
    mask, cell, amp, dly, ea, eb, em, ev, ledge, redge, got_up, got_dn, mask_up, mask_dn, got_l, got_r, corner,
    samp_own, samp_all, amp_t, high_t, low_t, sb, hist, outbox, scales, scale_out, inbox, inscales, units,
    entered, loads, store, halo_send, halo_recv, samp_send, samp_recv, bin_send, bin_recv, sc_send, sc_recv,
):
    b = lax.axis_index("box")
    p = lax.axis_index("panel")
    has_u, has_d, has_l, has_r = b > 0, b < BOX - 1, p > 0, p < PAN - 1
    diagonals = (
        (has_u & has_l, b - 1, p - 1),
        (has_u & has_r, b - 1, p + 1),
        (has_d & has_l, b + 1, p - 1),
        (has_d & has_r, b + 1, p + 1),
    )

    own_rows, own_cols = pl.ds(FIRST, ROWS), pl.ds(0, COLS)
    arrivals = [
        pltpu.make_async_copy(src, dst, loads.at[i])
        for i, (src, dst) in enumerate((
            (field_in, ea.at[own_rows, own_cols]), (visc_in, ev.at[own_rows, own_cols]),
            (mask_in, mask), (cell_in, cell), (amp_in, amp), (dly_in, dly),
        ))
    ]
    for copy in arrivals:
        copy.start()

    barrier = pltpu.get_barrier_semaphore()

    def greet(bb, pp):
        pl.semaphore_signal(barrier, inc=1, device_id=(bb, pp), device_id_type=MESH)

    for k in range(1, PAN):
        greet(b, lax.rem(p + k, PAN))
    y, z = b // SIDE, lax.rem(b, SIDE)
    row = [y * SIDE + lax.rem(z + k, SIDE) for k in range(1, SIDE)]
    for k in range(1, SIDE):
        greet(row[k - 1], p)
        greet(lax.rem(y + k, SIDE) * SIDE + z, p)
    expected = jnp.int32(PAN - 1 + 2 * (SIDE - 1))
    turns = ((has_u & (z == 0), b - 1, p), (has_d & (z == SIDE - 1), b + 1, p))
    for there, bb, pp in diagonals + turns:
        expected = expected + there.astype(jnp.int32)

        @pl.when(there)
        def _(bb=bb, pp=pp):
            greet(bb, pp)

    for buf in (ea, eb, ev, em):
        buf[0:8, :] = jnp.zeros((8, EXT_C), jnp.float32)
        buf[BOT + 8 :, :] = jnp.zeros((EXT_R - BOT - 8, EXT_C), jnp.float32)
    hist[...] = jnp.zeros_like(hist)
    samp_own[...] = jnp.zeros_like(samp_own)
    for copy in arrivals[:4]:
        copy.wait()

    lane = lax.broadcasted_iota(jnp.int32, (ROWS, 128), 1)
    fe, ve = ea[own_rows, :128], ev[own_rows, :128]
    me = mask[:, :128].astype(jnp.float32)
    ledge[...] = jnp.where(
        lane < 4, fe, jnp.where(lane < 8, roll(ve, 4, 1), jnp.where(lane < 12, roll(me, 8, 1), 0.0))
    )
    fe, ve = ea[own_rows, COLS - 128 : COLS], ev[own_rows, COLS - 128 : COLS]
    me = mask[:, COLS - 128 :].astype(jnp.float32)
    redge[...] = jnp.where(
        lane >= 124, fe, jnp.where(lane >= 120, roll(ve, -4, 1), jnp.where(lane >= 116, roll(me, -8, 1), 0.0))
    )
    em[own_rows, :COLS] = mask[...].astype(jnp.float32)
    for copy in arrivals[4:]:
        copy.wait()

    def turn(i, _):
        ps = pl.ds(pl.multiple_of(i * 128, 128), 128)
        for c in range(OBS // 128):
            cs = pl.ds(c * 128, 128)
            amp_t[cs, ps] = amp[ps, cs].astype(jnp.float32).T
            d = dly[ps, cs]
            low = d & 127
            r = (low * 79) >> 11
            high_t[cs, ps] = (r * 16 + (d >> 7)).astype(jnp.float32).T
            low_t[cs, ps] = (low - RADIX * r).astype(jnp.float32).T
        return 0

    lax.fori_loop(0, EARLY, turn, 0)

    def send(i, there, src, dst, bb, pp):
        copy = pltpu.make_async_remote_copy(
            src_ref=src, dst_ref=dst, send_sem=halo_send.at[i], recv_sem=halo_recv.at[i],
            device_id=(bb, pp), device_id_type=MESH,
        )
        return there, copy

    pl.semaphore_wait(barrier, expected)
    for other in row:
        pl.semaphore_signal(entered, inc=1, device_id=(other, p), device_id_type=MESH)

    lo8, hi8 = pl.ds(0, 8), pl.ds(ROWS - 8, 8)
    lo_own, hi_own = pl.ds(FIRST, 8), pl.ds(BOT - 8, 8)
    halos = (
        (send(0, has_u, ea.at[lo_own, own_cols], got_dn.at[0], b - 1, p), has_d),
        (send(1, has_u, ev.at[lo_own, own_cols], got_dn.at[1], b - 1, p), has_d),
        (send(2, has_u, mask.at[lo8], mask_dn, b - 1, p), has_d),
        (send(3, has_d, ea.at[hi_own, own_cols], got_up.at[0], b + 1, p), has_u),
        (send(4, has_d, ev.at[hi_own, own_cols], got_up.at[1], b + 1, p), has_u),
        (send(5, has_d, mask.at[hi8], mask_up, b + 1, p), has_u),
        (send(6, has_l, ledge, got_r, b, p - 1), has_r),
        (send(7, has_r, redge, got_l, b, p + 1), has_l),
        (send(8, has_d & has_r, redge.at[hi8], corner.at[0], b + 1, p + 1), has_u & has_l),
        (send(9, has_d & has_l, ledge.at[hi8], corner.at[1], b + 1, p - 1), has_u & has_r),
        (send(10, has_u & has_r, redge.at[lo8], corner.at[2], b - 1, p + 1), has_d & has_l),
        (send(11, has_u & has_l, ledge.at[lo8], corner.at[3], b - 1, p - 1), has_d & has_r),
    )
    for (there, copy), _ in halos:
        pl.when(there)(copy.start)

    def blank(flag, ref):
        @pl.when(jnp.logical_not(flag))
        def _():
            ref[...] = jnp.zeros(ref.shape, ref.dtype)

    blank(has_d, got_dn)
    blank(has_d, mask_dn)
    blank(has_u, got_up)
    blank(has_u, mask_up)
    blank(has_r, got_r)
    blank(has_l, got_l)
    blank(has_u & has_l, corner.at[0])
    blank(has_u & has_r, corner.at[1])
    blank(has_d & has_l, corner.at[2])
    blank(has_d & has_r, corner.at[3])

    lax.fori_loop(EARLY, PANELS // 128, turn, 0)

    for (there, copy), comes in halos:
        pl.when(comes)(copy.wait_recv)
        pl.when(there)(copy.wait_send)

    def side(left, right, shift, lane):
        return jnp.where(
            lane < 4, roll(right, -shift, 1), jnp.where(lane >= 124, roll(left, shift, 1), 0.0)
        )

    gl, gr = got_l[...], got_r[...]
    ea[FIRST:BOT, COLS:] = side(gl, gr, 0, lane)
    ev[FIRST:BOT, COLS:] = side(gl, gr, 4, lane)
    em[FIRST:BOT, COLS:] = side(gl, gr, 8, lane)
    lane8 = lax.broadcasted_iota(jnp.int32, (8, 128), 1)
    sub8 = lax.broadcasted_iota(jnp.int32, (8, 128), 0)
    sub_w = lax.broadcasted_iota(jnp.int32, (8, COLS), 0)
    for start, keep, keep_w, got, gmask, cl, cr in (
        (TOP, sub8 >= 4, sub_w >= 4, got_up, mask_up, corner[0], corner[1]),
        (BOT, sub8 < 4, sub_w < 4, got_dn, mask_dn, corner[2], corner[3]),
    ):
        rows = pl.ds(start, 8)
        ea[rows, :COLS] = jnp.where(keep_w, got[0], 0.0)
        ev[rows, :COLS] = jnp.where(keep_w, got[1], 0.0)
        em[rows, :COLS] = jnp.where(keep_w, gmask[...].astype(jnp.float32), 0.0)
        ea[rows, COLS:] = jnp.where(keep, side(cl, cr, 0, lane8), 0.0)
        ev[rows, COLS:] = jnp.where(keep, side(cl, cr, 4, lane8), 0.0)
        em[rows, COLS:] = jnp.where(keep, side(cl, cr, 8, lane8), 0.0)

    crow = cell[...] >> 9
    ccol = cell[...] & (COLS - 1)
    pick_c = jnp.where(
        lax.broadcasted_iota(jnp.int32, (COLS, OWN), 0) == ccol, 1.0, 0.0
    ).astype(jnp.bfloat16)
    pick_r = lax.broadcasted_iota(jnp.int32, (ROWS, OWN), 0) == crow
    for step in range(STEPS):
        src, dst = (ea, eb) if step % 2 == 0 else (eb, ea)

        def advance(i, _, src=src, dst=dst):
            at = pl.multiple_of(TOP + STRIP * i, 8)
            rows = pl.ds(at, STRIP)
            wide = src[pl.ds(pl.multiple_of(at - 8, 8), STRIP + 16), :]
            center = wide[8 : STRIP + 8]
            west = roll(wide, 1, 0)[8 : STRIP + 8]
            east = roll(wide, -1, 0)[8 : STRIP + 8]
            south = roll(center, 1, 1)
            north = roll(center, -1, 1)
            dx, dy = east - west, north - south
            square = dx * dx + dy * dy
            h = square * lax.rsqrt(jnp.maximum(square, 1e-30))
            viscosity = ev[rows, :] + 0.05 * h / (2.0 + h)
            spread = (east + west) + (north + south) - 4.0 * center
            update = 0.75 * center + 0.15 * west + 0.1 * south + viscosity * spread
            dst[rows, :] = em[rows, :] * update
            return 0

        lax.fori_loop(0, (EXT_R - 16) // STRIP, advance, 0)
        found = jnp.dot(
            dst[FIRST:BOT, :COLS].astype(jnp.bfloat16), pick_c, preferred_element_type=jnp.float32
        )
        samp_own[step : step + 1, :] = jnp.sum(jnp.where(pick_r, found, 0.0), axis=0, keepdims=True)

    out = pltpu.make_async_copy(ea.at[own_rows, own_cols], field_out, store)
    out.start()

    mine = pl.ds(pl.multiple_of(p * OWN, OWN), OWN)
    samp_all[:, mine] = samp_own[...]

    def samp_copy(k):
        to = lax.rem(p + k, PAN)
        return pltpu.make_async_remote_copy(
            src_ref=samp_own, dst_ref=samp_all.at[:, mine], send_sem=samp_send.at[k],
            recv_sem=samp_recv.at[p], device_id=(b, to), device_id_type=MESH,
        )

    def samp_arrival(k):
        frm = lax.rem(p + k, PAN)
        return pltpu.make_async_remote_copy(
            src_ref=samp_own, dst_ref=samp_all.at[:, pl.ds(pl.multiple_of(frm * OWN, OWN), OWN)],
            send_sem=samp_send.at[k], recv_sem=samp_recv.at[frm], device_id=(b, frm), device_id_type=MESH,
        )

    for k in range(1, PAN):
        samp_copy(k).start()
    for k in range(1, PAN):
        samp_arrival(k).wait_recv()
    for t in range(STEPS):
        sb[t] = jnp.broadcast_to(samp_all[t : t + 1, :], (16, PANELS)).astype(jnp.bfloat16)

    io16 = lax.broadcasted_iota(jnp.int32, (16, KT), 0).astype(jnp.float32)
    lane16 = lax.broadcasted_iota(jnp.int32, (16, 128), 1)
    sub16 = lax.broadcasted_iota(jnp.int32, (16, 128), 0)
    zero = jnp.zeros((16, KT), jnp.bfloat16)

    def bin_group(first, slot):
        acc = None
        for k in range(PANELS // KT):
            ks = pl.ds(k * KT, KT)
            ss = [sb[t, :, ks] for t in range(STEPS)]
            lhs, rhs = [], []
            for i in range(STACK):
                o = pl.ds(first + i, 1)
                hb = jnp.broadcast_to(high_t[o, ks], (16, KT)).astype(jnp.bfloat16)
                ab = jnp.broadcast_to(amp_t[o, ks], (16, KT)).astype(jnp.bfloat16)
                lb = jnp.broadcast_to(low_t[o, ks], (16, KT)).astype(jnp.bfloat16)
                for j in range(HIGH // 16):
                    lhs.append(jnp.where(hb == (io16 + 16 * j).astype(jnp.bfloat16), ab, zero))
                for j in range(LOW // 16):
                    v = zero
                    for t in range(STEPS):
                        v = jnp.where(lb == (io16 + (16 * j - t)).astype(jnp.bfloat16), ss[t], v)
                    rhs.append(v)
            part = lax.dot_general(
                jnp.concatenate(lhs, 0), jnp.concatenate(rhs, 0), (((1,), (1,)), ((), ())),
                preferred_element_type=jnp.float32,
            )
            acc = part if acc is None else acc + part
        for i in range(STACK):
            total = None
            for r in range(PARTS):
                blk = acc[i * HIGH + 16 * r : i * HIGH + 16 * r + 16, :]
                blk = jnp.where((lane16 >= LOW * i) & (lane16 < LOW * i + LOW), blk, 0.0)
                if (RADIX * r - LOW * i) % 128:
                    blk = roll(blk, RADIX * r - LOW * i, 1)
                if r == PARTS - 1:
                    over = jnp.where((lane16 < 8) & (sub16 < 15), blk, 0.0)
                    blk = jnp.where(lane16 < 8, 0.0, blk) + roll(over, 1, 0)
                total = blk if total is None else total + blk
            hist[pl.ds(slot + i, 16, stride=PITCH), :] = total

    def bin_copy(k, h):
        to = lax.rem(b + k, BOX)
        rows = pl.ds(pl.multiple_of(h * HALF, HALF), HALF)
        return pltpu.make_async_remote_copy(
            src_ref=outbox.at[to, rows], dst_ref=inbox.at[b, rows], send_sem=bin_send.at[k],
            recv_sem=bin_recv.at[b], device_id=(to, p), device_id_type=MESH,
        )

    def bin_whole(k):
        frm = lax.rem(b + k, BOX)
        return pltpu.make_async_remote_copy(
            src_ref=outbox.at[frm], dst_ref=inbox.at[frm], send_sem=bin_send.at[k],
            recv_sem=bin_recv.at[frm], device_id=(frm, p), device_id_type=MESH,
        )

    def scale_copy(k):
        to = lax.rem(b + k, BOX)
        return pltpu.make_async_remote_copy(
            src_ref=scale_out.at[to], dst_ref=inscales.at[b], send_sem=sc_send.at[k],
            recv_sem=sc_recv.at[b], device_id=(to, p), device_id_type=MESH,
        )

    def scale_arrival(k):
        frm = lax.rem(b + k, BOX)
        return pltpu.make_async_remote_copy(
            src_ref=scale_out.at[frm], dst_ref=inscales.at[frm], send_sem=sc_send.at[k],
            recv_sem=sc_recv.at[frm], device_id=(frm, p), device_id_type=MESH,
        )

    def pack(h, part):
        rows = pl.ds(pl.multiple_of(h * HALF, HALF), HALF)
        for q in range(BOX):
            at = q * PITCH + part * HALF
            x = hist[at : at + HALF, :]
            most = jnp.max(jnp.max(jnp.abs(x), axis=0, keepdims=True), axis=1, keepdims=True)
            most = jnp.maximum(jnp.broadcast_to(most, (1, 128)), 1e-30)
            unit = (most * (1.0 / TOPINT)).astype(jnp.bfloat16).astype(jnp.float32)
            y = jnp.floor(x * (1.0 / unit) + 0.5)
            outbox[q, rows, :] = y.astype(jnp.int32).astype(jnp.int16)
            scales[q, pl.ds(h, 1), :] = unit

    def post(h):
        for k in ORDER:
            bin_copy(k, h).start()

    def chunk(c, _):
        before = jnp.maximum(2 * c - 1, 1)
        pack(before, 1)
        for u in range(HALF // STACK):
            bin_group(c * CHUNK + u * STACK, u * STACK)
        pack(2 * c, 0)
        for u in range(HALF // STACK, CHUNK // STACK):
            bin_group(c * CHUNK + u * STACK, u * STACK)

        @pl.when(c > 0)
        def _():
            post(before)

        post(2 * c)
        return 0

    pl.semaphore_wait(entered, SIDE - 1)
    lax.fori_loop(0, CHUNKS, chunk, 0)
    pack(HALVES - 1, 1)
    post(HALVES - 1)
    scale_out[...] = scales[...].astype(jnp.bfloat16)
    for k in ORDER:
        scale_copy(k).start()
    inscales[b] = scale_out[b]
    inbox[b] = outbox[b]

    def arrive(k, _):
        scale_arrival(k).wait_recv()
        bin_whole(k).wait_recv()
        return 0

    lax.fori_loop(1, BOX, arrive, 0)

    for s in range(BOX):
        units[s] = inscales[s].astype(jnp.float32)

    def gather(h, _):
        rows = pl.ds(pl.multiple_of(h * HALF, HALF), HALF)
        total = None
        for s in range(BOX):
            x = inbox[s, rows, :].astype(jnp.int32).astype(jnp.float32) * units[s, pl.ds(h, 1), :]
            total = x if total is None else total + x
        sig_out[rows, :] = total
        return 0

    lax.fori_loop(0, HALVES, gather, 0)

    out.wait()
    for k in range(1, PAN):
        samp_copy(k).wait_send()

    def sent(k, _):
        scale_copy(k).wait_send()
        bin_whole(k).wait_send()
        return 0

    lax.fori_loop(1, BOX, sent, 0)


def hand_over(field, signals, field_out, sig_out, sems):
    copies = (
        pltpu.make_async_copy(field, field_out, sems.at[0]),
        pltpu.make_async_copy(signals, sig_out, sems.at[1]),
    )
    for copy in copies:
        copy.start()
    for copy in copies:
        copy.wait()


def on_device(field_start, fluid_mask, base_visc, panel_cell, amplitude, delay_bin):
    f32, bf16, i32 = jnp.float32, jnp.bfloat16, jnp.int32
    vmem = lambda shape, dtype=f32: pltpu.VMEM(shape, dtype)
    dma = lambda *shape: pltpu.SemaphoreType.DMA(shape)
    scratch = [
        vmem((ROWS, COLS), i32), vmem((1, OWN), i32), vmem((PANELS, OBS), bf16), vmem((PANELS, OBS), i32),
        vmem((EXT_R, EXT_C)), vmem((EXT_R, EXT_C)), vmem((EXT_R, EXT_C)), vmem((EXT_R, EXT_C)),
        vmem((ROWS, 128)), vmem((ROWS, 128)),
        vmem((2, 8, COLS)), vmem((2, 8, COLS)), vmem((8, COLS), i32), vmem((8, COLS), i32),
        vmem((ROWS, 128)), vmem((ROWS, 128)), vmem((4, 8, 128)),
        vmem((8, OWN)), vmem((8, PANELS)),
        vmem((OBS, PANELS)), vmem((OBS, PANELS)), vmem((OBS, PANELS)),
        vmem((STEPS, 16, PANELS), bf16),
        vmem((BOX * PITCH, 128)),
        vmem((BOX, OBS, 128), jnp.int16), vmem((BOX, HALVES, 128)), vmem((BOX, HALVES, 128), bf16),
        vmem((BOX, OBS, 128), jnp.int16), vmem((BOX, HALVES, 128), bf16), vmem((BOX, HALVES, 128)),
        pltpu.SemaphoreType.REGULAR, dma(6), pltpu.SemaphoreType.DMA, dma(12), dma(12), dma(PAN), dma(PAN), dma(BOX), dma(BOX), dma(BOX), dma(BOX),
    ]
    field, signals = pl.pallas_call(
        kernel,
        out_shape=(
            pltpu.VMEM((ROWS, COLS), f32),
            pltpu.VMEM((OBS, NB // BOX), f32),
        ),
        in_specs=[pl.BlockSpec(memory_space=pl.ANY)] * 6,
        out_specs=(pl.BlockSpec(memory_space=pl.ANY), pl.BlockSpec(memory_space=pltpu.VMEM)),
        scratch_shapes=scratch,
        compiler_params=pltpu.CompilerParams(
            collective_id=0, has_side_effects=True, vmem_limit_bytes=56 * 2**20
        ),
    )(field_start, fluid_mask, base_visc, panel_cell.reshape(1, OWN), amplitude, delay_bin)
    return pl.pallas_call(
        hand_over,
        out_shape=(
            jax.ShapeDtypeStruct((ROWS, COLS), f32),
            jax.ShapeDtypeStruct((OBS, NB // BOX), f32),
        ),
        in_specs=[pl.BlockSpec(memory_space=pltpu.VMEM)] * 2,
        out_specs=(pl.BlockSpec(memory_space=pl.ANY),) * 2,
        scratch_shapes=[dma(2)],
        compiler_params=pltpu.CompilerParams(vmem_limit_bytes=4 * 2**20),
    )(field, signals)


def solution(mesh):
    placed = (
        P("box", "panel"),
        P("box", "panel"),
        P("box", "panel"),
        P(("box", "panel")),
        P("box", "panel"),
        P("box", "panel"),
    )
    return jax.shard_map(
        on_device,
        mesh=mesh,
        in_specs=placed,
        out_specs=(P("box", "panel"), P("panel", "box")),
        check_vma=False,
    )
```

```python
import functools

import jax
import jax.numpy as jnp
from jax import lax
from jax.experimental import pallas as pl
from jax.experimental.pallas import tpu as pltpu
from jax.sharding import PartitionSpec as P

MESH = pl.DeviceIdType.MESH
STEPS = 4
NB = 2048
BOX = 16
SIDE = 4
PAN = 8
ROWS, COLS = 256, 512
PANELS, OBS, OWN = 1024, 512, 128
TOP, FIRST, BOT, EXT_R, EXT_C = 8, 16, 272, 304, 640
STRIP = 96
RADIX, PARTS, HIGH, LOW = 26, 5, 80, 32
STACK = 4
KT = 256
CHUNK = 64
CHUNKS = OBS // CHUNK
HALF = CHUNK // 2
HALVES = OBS // HALF
PITCH = CHUNK + 8
TOPINT = 32000.0
ORDER = (10, 9, 11, 6, 14, 8, 2, 5, 7, 13, 15, 12, 4, 3, 1)


def roll(x, shift, axis):
    return pltpu.roll(x, shift % x.shape[axis], axis)


def kernel(
    field_in, mask_in, visc_in, cell_in, amp_in, dly_in, field_out, sig_out,
    mask, cell, amp, dly, ea, eb, em, ev, ledge, redge, got_up, got_dn, mask_up, mask_dn, got_l, got_r, corner,
    samp_own, samp_all, amp_t, high_t, low_t, sb, hist, outbox, scales, scale_out, inbox, inscales, units,
    entered, loads, store, halo_send, halo_recv, samp_send, samp_recv, bin_send, bin_recv, sc_send, sc_recv,
):
    b = lax.axis_index("box")
    p = lax.axis_index("panel")
    has_u, has_d, has_l, has_r = b > 0, b < BOX - 1, p > 0, p < PAN - 1
    diagonals = (
        (has_u & has_l, b - 1, p - 1),
        (has_u & has_r, b - 1, p + 1),
        (has_d & has_l, b + 1, p - 1),
        (has_d & has_r, b + 1, p + 1),
    )

    own_rows, own_cols = pl.ds(FIRST, ROWS), pl.ds(0, COLS)
    arrivals = [
        pltpu.make_async_copy(src, dst, loads.at[i])
        for i, (src, dst) in enumerate((
            (field_in, ea.at[own_rows, own_cols]), (visc_in, ev.at[own_rows, own_cols]),
            (mask_in, mask), (cell_in, cell), (amp_in, amp), (dly_in, dly),
        ))
    ]
    for copy in arrivals:
        copy.start()

    barrier = pltpu.get_barrier_semaphore()

    def greet(bb, pp):
        pl.semaphore_signal(barrier, inc=1, device_id=(bb, pp), device_id_type=MESH)

    for k in range(1, PAN):
        greet(b, lax.rem(p + k, PAN))
    y, z = b // SIDE, lax.rem(b, SIDE)
    row = [y * SIDE + lax.rem(z + k, SIDE) for k in range(1, SIDE)]
    for k in range(1, SIDE):
        greet(row[k - 1], p)
        greet(lax.rem(y + k, SIDE) * SIDE + z, p)
    expected = jnp.int32(PAN - 1 + 2 * (SIDE - 1))
    turns = ((has_u & (z == 0), b - 1, p), (has_d & (z == SIDE - 1), b + 1, p))
    for there, bb, pp in diagonals + turns:
        expected = expected + there.astype(jnp.int32)

        @pl.when(there)
        def _(bb=bb, pp=pp):
            greet(bb, pp)

    for buf in (ea, eb, ev, em):
        buf[0:8, :] = jnp.zeros((8, EXT_C), jnp.float32)
        buf[BOT + 8 :, :] = jnp.zeros((EXT_R - BOT - 8, EXT_C), jnp.float32)
    hist[...] = jnp.zeros_like(hist)
    samp_own[...] = jnp.zeros_like(samp_own)
    for copy in arrivals[:4]:
        copy.wait()

    lane = lax.broadcasted_iota(jnp.int32, (ROWS, 128), 1)
    fe, ve = ea[own_rows, :128], ev[own_rows, :128]
    me = mask[:, :128].astype(jnp.float32)
    ledge[...] = jnp.where(
        lane < 4, fe, jnp.where(lane < 8, roll(ve, 4, 1), jnp.where(lane < 12, roll(me, 8, 1), 0.0))
    )
    fe, ve = ea[own_rows, COLS - 128 : COLS], ev[own_rows, COLS - 128 : COLS]
    me = mask[:, COLS - 128 :].astype(jnp.float32)
    redge[...] = jnp.where(
        lane >= 124, fe, jnp.where(lane >= 120, roll(ve, -4, 1), jnp.where(lane >= 116, roll(me, -8, 1), 0.0))
    )
    em[own_rows, :COLS] = mask[...].astype(jnp.float32)

    def turn(i, _):
        ps = pl.ds(pl.multiple_of(i * 128, 128), 128)
        for c in range(OBS // 128):
            cs = pl.ds(c * 128, 128)
            amp_t[cs, ps] = amp[ps, cs].astype(jnp.float32).T
            d = dly[ps, cs]
            low = d & 127
            r = (low * 79) >> 11
            high_t[cs, ps] = (r * 16 + (d >> 7)).astype(jnp.float32).T
            low_t[cs, ps] = (low - RADIX * r).astype(jnp.float32).T
        return 0

    def send(i, there, src, dst, bb, pp):
        copy = pltpu.make_async_remote_copy(
            src_ref=src, dst_ref=dst, send_sem=halo_send.at[i], recv_sem=halo_recv.at[i],
            device_id=(bb, pp), device_id_type=MESH,
        )
        return there, copy

    pl.semaphore_wait(barrier, expected)
    for other in row:
        pl.semaphore_signal(entered, inc=1, device_id=(other, p), device_id_type=MESH)

    lo8, hi8 = pl.ds(0, 8), pl.ds(ROWS - 8, 8)
    lo_own, hi_own = pl.ds(FIRST, 8), pl.ds(BOT - 8, 8)
    halos = (
        (send(0, has_u, ea.at[lo_own, own_cols], got_dn.at[0], b - 1, p), has_d),
        (send(1, has_u, ev.at[lo_own, own_cols], got_dn.at[1], b - 1, p), has_d),
        (send(2, has_u, mask.at[lo8], mask_dn, b - 1, p), has_d),
        (send(3, has_d, ea.at[hi_own, own_cols], got_up.at[0], b + 1, p), has_u),
        (send(4, has_d, ev.at[hi_own, own_cols], got_up.at[1], b + 1, p), has_u),
        (send(5, has_d, mask.at[hi8], mask_up, b + 1, p), has_u),
        (send(6, has_l, ledge, got_r, b, p - 1), has_r),
        (send(7, has_r, redge, got_l, b, p + 1), has_l),
        (send(8, has_d & has_r, redge.at[hi8], corner.at[0], b + 1, p + 1), has_u & has_l),
        (send(9, has_d & has_l, ledge.at[hi8], corner.at[1], b + 1, p - 1), has_u & has_r),
        (send(10, has_u & has_r, redge.at[lo8], corner.at[2], b - 1, p + 1), has_d & has_l),
        (send(11, has_u & has_l, ledge.at[lo8], corner.at[3], b - 1, p - 1), has_d & has_r),
    )
    for (there, copy), _ in halos:
        pl.when(there)(copy.start)

    def blank(flag, ref):
        @pl.when(jnp.logical_not(flag))
        def _():
            ref[...] = jnp.zeros(ref.shape, ref.dtype)

    blank(has_d, got_dn)
    blank(has_d, mask_dn)
    blank(has_u, got_up)
    blank(has_u, mask_up)
    blank(has_r, got_r)
    blank(has_l, got_l)
    blank(has_u & has_l, corner.at[0])
    blank(has_u & has_r, corner.at[1])
    blank(has_d & has_l, corner.at[2])
    blank(has_d & has_r, corner.at[3])

    for copy in arrivals[4:]:
        copy.wait()
    lax.fori_loop(0, PANELS // 128, turn, 0)

    for (there, copy), comes in halos:
        pl.when(comes)(copy.wait_recv)
        pl.when(there)(copy.wait_send)

    def side(left, right, shift, lane):
        return jnp.where(
            lane < 4, roll(right, -shift, 1), jnp.where(lane >= 124, roll(left, shift, 1), 0.0)
        )

    gl, gr = got_l[...], got_r[...]
    ea[FIRST:BOT, COLS:] = side(gl, gr, 0, lane)
    ev[FIRST:BOT, COLS:] = side(gl, gr, 4, lane)
    em[FIRST:BOT, COLS:] = side(gl, gr, 8, lane)
    lane8 = lax.broadcasted_iota(jnp.int32, (8, 128), 1)
    sub8 = lax.broadcasted_iota(jnp.int32, (8, 128), 0)
    sub_w = lax.broadcasted_iota(jnp.int32, (8, COLS), 0)
    for start, keep, keep_w, got, gmask, cl, cr in (
        (TOP, sub8 >= 4, sub_w >= 4, got_up, mask_up, corner[0], corner[1]),
        (BOT, sub8 < 4, sub_w < 4, got_dn, mask_dn, corner[2], corner[3]),
    ):
        rows = pl.ds(start, 8)
        ea[rows, :COLS] = jnp.where(keep_w, got[0], 0.0)
        ev[rows, :COLS] = jnp.where(keep_w, got[1], 0.0)
        em[rows, :COLS] = jnp.where(keep_w, gmask[...].astype(jnp.float32), 0.0)
        ea[rows, COLS:] = jnp.where(keep, side(cl, cr, 0, lane8), 0.0)
        ev[rows, COLS:] = jnp.where(keep, side(cl, cr, 4, lane8), 0.0)
        em[rows, COLS:] = jnp.where(keep, side(cl, cr, 8, lane8), 0.0)

    crow = cell[...] >> 9
    ccol = cell[...] & (COLS - 1)
    pick_c = jnp.where(
        lax.broadcasted_iota(jnp.int32, (COLS, OWN), 0) == ccol, 1.0, 0.0
    ).astype(jnp.bfloat16)
    pick_r = lax.broadcasted_iota(jnp.int32, (ROWS, OWN), 0) == crow
    for step in range(STEPS):
        src, dst = (ea, eb) if step % 2 == 0 else (eb, ea)

        def advance(i, _, src=src, dst=dst):
            at = pl.multiple_of(TOP + STRIP * i, 8)
            rows = pl.ds(at, STRIP)
            wide = src[pl.ds(pl.multiple_of(at - 8, 8), STRIP + 16), :]
            center = wide[8 : STRIP + 8]
            west = roll(wide, 1, 0)[8 : STRIP + 8]
            east = roll(wide, -1, 0)[8 : STRIP + 8]
            south = roll(center, 1, 1)
            north = roll(center, -1, 1)
            dx, dy = east - west, north - south
            square = dx * dx + dy * dy
            h = square * lax.rsqrt(jnp.maximum(square, 1e-30))
            viscosity = ev[rows, :] + 0.05 * h / (2.0 + h)
            spread = (east + west) + (north + south) - 4.0 * center
            update = 0.75 * center + 0.15 * west + 0.1 * south + viscosity * spread
            dst[rows, :] = em[rows, :] * update
            return 0

        lax.fori_loop(0, (EXT_R - 16) // STRIP, advance, 0)
        found = jnp.dot(
            dst[FIRST:BOT, :COLS].astype(jnp.bfloat16), pick_c, preferred_element_type=jnp.float32
        )
        samp_own[step : step + 1, :] = jnp.sum(jnp.where(pick_r, found, 0.0), axis=0, keepdims=True)

    out = pltpu.make_async_copy(ea.at[own_rows, own_cols], field_out, store)
    out.start()

    mine = pl.ds(pl.multiple_of(p * OWN, OWN), OWN)
    samp_all[:, mine] = samp_own[...]

    def samp_copy(k):
        to = lax.rem(p + k, PAN)
        return pltpu.make_async_remote_copy(
            src_ref=samp_own, dst_ref=samp_all.at[:, mine], send_sem=samp_send.at[k],
            recv_sem=samp_recv.at[p], device_id=(b, to), device_id_type=MESH,
        )

    def samp_arrival(k):
        frm = lax.rem(p + k, PAN)
        return pltpu.make_async_remote_copy(
            src_ref=samp_own, dst_ref=samp_all.at[:, pl.ds(pl.multiple_of(frm * OWN, OWN), OWN)],
            send_sem=samp_send.at[k], recv_sem=samp_recv.at[frm], device_id=(b, frm), device_id_type=MESH,
        )

    for k in range(1, PAN):
        samp_copy(k).start()
    for k in range(1, PAN):
        samp_arrival(k).wait_recv()
    for t in range(STEPS):
        sb[t] = jnp.broadcast_to(samp_all[t : t + 1, :], (16, PANELS)).astype(jnp.bfloat16)

    io16 = lax.broadcasted_iota(jnp.int32, (16, KT), 0).astype(jnp.float32)
    lane16 = lax.broadcasted_iota(jnp.int32, (16, 128), 1)
    sub16 = lax.broadcasted_iota(jnp.int32, (16, 128), 0)
    zero = jnp.zeros((16, KT), jnp.bfloat16)

    def bin_group(first, slot):
        acc = None
        for k in range(PANELS // KT):
            ks = pl.ds(k * KT, KT)
            ss = [sb[t, :, ks] for t in range(STEPS)]
            lhs, rhs = [], []
            for i in range(STACK):
                o = pl.ds(first + i, 1)
                hb = jnp.broadcast_to(high_t[o, ks], (16, KT)).astype(jnp.bfloat16)
                ab = jnp.broadcast_to(amp_t[o, ks], (16, KT)).astype(jnp.bfloat16)
                lb = jnp.broadcast_to(low_t[o, ks], (16, KT)).astype(jnp.bfloat16)
                for j in range(HIGH // 16):
                    lhs.append(jnp.where(hb == (io16 + 16 * j).astype(jnp.bfloat16), ab, zero))
                for j in range(LOW // 16):
                    v = zero
                    for t in range(STEPS):
                        v = jnp.where(lb == (io16 + (16 * j - t)).astype(jnp.bfloat16), ss[t], v)
                    rhs.append(v)
            part = lax.dot_general(
                jnp.concatenate(lhs, 0), jnp.concatenate(rhs, 0), (((1,), (1,)), ((), ())),
                preferred_element_type=jnp.float32,
            )
            acc = part if acc is None else acc + part
        for i in range(STACK):
            total = None
            for r in range(PARTS):
                blk = acc[i * HIGH + 16 * r : i * HIGH + 16 * r + 16, :]
                blk = jnp.where((lane16 >= LOW * i) & (lane16 < LOW * i + LOW), blk, 0.0)
                if (RADIX * r - LOW * i) % 128:
                    blk = roll(blk, RADIX * r - LOW * i, 1)
                if r == PARTS - 1:
                    over = jnp.where((lane16 < 8) & (sub16 < 15), blk, 0.0)
                    blk = jnp.where(lane16 < 8, 0.0, blk) + roll(over, 1, 0)
                total = blk if total is None else total + blk
            hist[pl.ds(slot + i, 16, stride=PITCH), :] = total

    def bin_copy(k, h):
        to = lax.rem(b + k, BOX)
        rows = pl.ds(pl.multiple_of(h * HALF, HALF), HALF)
        return pltpu.make_async_remote_copy(
            src_ref=outbox.at[to, rows], dst_ref=inbox.at[b, rows], send_sem=bin_send.at[k],
            recv_sem=bin_recv.at[b], device_id=(to, p), device_id_type=MESH,
        )

    def bin_whole(k):
        frm = lax.rem(b + k, BOX)
        return pltpu.make_async_remote_copy(
            src_ref=outbox.at[frm], dst_ref=inbox.at[frm], send_sem=bin_send.at[k],
            recv_sem=bin_recv.at[frm], device_id=(frm, p), device_id_type=MESH,
        )

    def scale_copy(k):
        to = lax.rem(b + k, BOX)
        return pltpu.make_async_remote_copy(
            src_ref=scale_out.at[to], dst_ref=inscales.at[b], send_sem=sc_send.at[k],
            recv_sem=sc_recv.at[b], device_id=(to, p), device_id_type=MESH,
        )

    def scale_arrival(k):
        frm = lax.rem(b + k, BOX)
        return pltpu.make_async_remote_copy(
            src_ref=scale_out.at[frm], dst_ref=inscales.at[frm], send_sem=sc_send.at[k],
            recv_sem=sc_recv.at[frm], device_id=(frm, p), device_id_type=MESH,
        )

    def pack(h, part):
        rows = pl.ds(pl.multiple_of(h * HALF, HALF), HALF)
        for q in range(BOX):
            at = q * PITCH + part * HALF
            x = hist[at : at + HALF, :]
            most = jnp.max(jnp.max(jnp.abs(x), axis=0, keepdims=True), axis=1, keepdims=True)
            most = jnp.maximum(jnp.broadcast_to(most, (1, 128)), 1e-30)
            unit = (most * (1.0 / TOPINT)).astype(jnp.bfloat16).astype(jnp.float32)
            y = jnp.floor(x * (1.0 / unit) + 0.5)
            outbox[q, rows, :] = y.astype(jnp.int32).astype(jnp.int16)
            scales[q, pl.ds(h, 1), :] = unit

    def post(h):
        for k in ORDER:
            bin_copy(k, h).start()

    def chunk(c, _):
        before = jnp.maximum(2 * c - 1, 1)
        pack(before, 1)
        for u in range(HALF // STACK):
            bin_group(c * CHUNK + u * STACK, u * STACK)
        pack(2 * c, 0)
        for u in range(HALF // STACK, CHUNK // STACK):
            bin_group(c * CHUNK + u * STACK, u * STACK)

        @pl.when(c > 0)
        def _():
            post(before)

        post(2 * c)
        return 0

    pl.semaphore_wait(entered, SIDE - 1)
    lax.fori_loop(0, CHUNKS, chunk, 0)
    pack(HALVES - 1, 1)
    post(HALVES - 1)
    scale_out[...] = scales[...].astype(jnp.bfloat16)
    for k in ORDER:
        scale_copy(k).start()
    inscales[b] = scale_out[b]
    inbox[b] = outbox[b]

    def arrive(k, _):
        scale_arrival(k).wait_recv()
        bin_whole(k).wait_recv()
        return 0

    lax.fori_loop(1, BOX, arrive, 0)

    for s in range(BOX):
        units[s] = inscales[s].astype(jnp.float32)

    def gather(h, _):
        rows = pl.ds(pl.multiple_of(h * HALF, HALF), HALF)
        total = None
        for s in range(BOX):
            x = inbox[s, rows, :].astype(jnp.int32).astype(jnp.float32) * units[s, pl.ds(h, 1), :]
            total = x if total is None else total + x
        sig_out[rows, :] = total
        return 0

    lax.fori_loop(0, HALVES, gather, 0)

    out.wait()
    for k in range(1, PAN):
        samp_copy(k).wait_send()

    def sent(k, _):
        scale_copy(k).wait_send()
        bin_whole(k).wait_send()
        return 0

    lax.fori_loop(1, BOX, sent, 0)


def hand_over(field, signals, field_out, sig_out, sems):
    copies = (
        pltpu.make_async_copy(field, field_out, sems.at[0]),
        pltpu.make_async_copy(signals, sig_out, sems.at[1]),
    )
    for copy in copies:
        copy.start()
    for copy in copies:
        copy.wait()


def on_device(field_start, fluid_mask, base_visc, panel_cell, amplitude, delay_bin):
    f32, bf16, i32 = jnp.float32, jnp.bfloat16, jnp.int32
    vmem = lambda shape, dtype=f32: pltpu.VMEM(shape, dtype)
    dma = lambda *shape: pltpu.SemaphoreType.DMA(shape)
    scratch = [
        vmem((ROWS, COLS), i32), vmem((1, OWN), i32), vmem((PANELS, OBS), bf16), vmem((PANELS, OBS), i32),
        vmem((EXT_R, EXT_C)), vmem((EXT_R, EXT_C)), vmem((EXT_R, EXT_C)), vmem((EXT_R, EXT_C)),
        vmem((ROWS, 128)), vmem((ROWS, 128)),
        vmem((2, 8, COLS)), vmem((2, 8, COLS)), vmem((8, COLS), i32), vmem((8, COLS), i32),
        vmem((ROWS, 128)), vmem((ROWS, 128)), vmem((4, 8, 128)),
        vmem((8, OWN)), vmem((8, PANELS)),
        vmem((OBS, PANELS)), vmem((OBS, PANELS)), vmem((OBS, PANELS)),
        vmem((STEPS, 16, PANELS), bf16),
        vmem((BOX * PITCH, 128)),
        vmem((BOX, OBS, 128), jnp.int16), vmem((BOX, HALVES, 128)), vmem((BOX, HALVES, 128), bf16),
        vmem((BOX, OBS, 128), jnp.int16), vmem((BOX, HALVES, 128), bf16), vmem((BOX, HALVES, 128)),
        pltpu.SemaphoreType.REGULAR, dma(6), pltpu.SemaphoreType.DMA, dma(12), dma(12), dma(PAN), dma(PAN), dma(BOX), dma(BOX), dma(BOX), dma(BOX),
    ]
    field, signals = pl.pallas_call(
        kernel,
        out_shape=(
            pltpu.VMEM((ROWS, COLS), f32),
            pltpu.VMEM((OBS, NB // BOX), f32),
        ),
        in_specs=[pl.BlockSpec(memory_space=pl.ANY)] * 6,
        out_specs=(pl.BlockSpec(memory_space=pl.ANY), pl.BlockSpec(memory_space=pltpu.VMEM)),
        scratch_shapes=scratch,
        compiler_params=pltpu.CompilerParams(
            collective_id=0, has_side_effects=True, vmem_limit_bytes=56 * 2**20
        ),
    )(field_start, fluid_mask, base_visc, panel_cell.reshape(1, OWN), amplitude, delay_bin)
    return pl.pallas_call(
        hand_over,
        out_shape=(
            jax.ShapeDtypeStruct((ROWS, COLS), f32),
            jax.ShapeDtypeStruct((OBS, NB // BOX), f32),
        ),
        in_specs=[pl.BlockSpec(memory_space=pltpu.VMEM)] * 2,
        out_specs=(pl.BlockSpec(memory_space=pl.ANY),) * 2,
        scratch_shapes=[dma(2)],
        compiler_params=pltpu.CompilerParams(vmem_limit_bytes=4 * 2**20),
    )(field, signals)


def solution(mesh):
    placed = (
        P("box", "panel"),
        P("box", "panel"),
        P("box", "panel"),
        P(("box", "panel")),
        P("box", "panel"),
        P("box", "panel"),
    )
    return jax.shard_map(
        on_device,
        mesh=mesh,
        in_specs=placed,
        out_specs=(P("box", "panel"), P("panel", "box")),
        check_vma=False,
    )
```
